128 devices in a mesh: rep: 1, r: 4 (over x), s: 32 (over y, z, core).
Axes of the slice: x: 4, y: 4, z: 4, core: 2. Of those that a mesh axis runs over, the one named last changes fastest.
Arguments:
- x: bfloat16 [128, 2048, 1280], P(('rep', 'r', 's'))
- dy: bfloat16 [128, 2048, 1280], P(('rep', 'r', 's'))
- w_gate: bfloat16 [2, 1280, 4480], P(None, 's')
- w_up: bfloat16 [2, 1280, 4480], P(None, 's')
- w_down: bfloat16 [2, 4480, 1280], P(None, 's')
- m_w_gate: float32 [2, 1280, 4480], P(None, 's')
- m_w_up: float32 [2, 1280, 4480], P(None, 's')
- m_w_down: float32 [2, 4480, 1280], P(None, 's')
- v_w_gate: float32 [2, 1280, 4480], P(None, 's')
- v_w_up: float32 [2, 1280, 4480], P(None, 's')
- v_w_down: float32 [2, 4480, 1280], P(None, 's')
Outputs:
- output 1: bfloat16 [2, 1280, 4480], P('rep', 's')
- output 2: bfloat16 [2, 1280, 4480], P('rep', 's')
- output 3: bfloat16 [2, 4480, 1280], P('rep', 's')
- output 4: float32 [2, 1280, 4480], P('rep', 's')
- output 5: float32 [2, 1280, 4480], P('rep', 's')
- output 6: float32 [2, 4480, 1280], P('rep', 's')
- output 7: float32 [2, 1280, 4480], P('rep', 's')
- output 8: float32 [2, 1280, 4480], P('rep', 's')
- output 9: float32 [2, 4480, 1280], P('rep', 's')
All inputs are finite; a program needn't handle non-finite values.
Results may differ from the reference program's by a relative error of at most 0.022.
Values are sent between devices in bfloat16 or wider.
A program may use at most 1.5 GiB of HBM per device.

```python
import jax
import jax.numpy as jnp
from jax import lax

SEQUENCES = 128
TOKENS = 2048
D = 1280
FF = 4480
LAYERS = 2
NAMES = ("w_gate", "w_up", "w_down")
SHAPES = {"w_gate": (LAYERS, D, FF), "w_up": (LAYERS, D, FF), "w_down": (LAYERS, FF, D)}


def bump(key, n, height):
    away = (jnp.arange(n, dtype=jnp.int32) - jax.random.randint(key, (), 0, n, jnp.int32)) % n
    return jnp.where(away < n // 8, height, 1.0)


def together(key, own, strength):
    shared = jax.random.normal(key, own.shape[1:], jnp.float32)
    return (own + strength * shared) * lax.rsqrt(1 + strength * strength)


def setup_inputs(seed: int = 0, part: int = 0) -> dict:
    kx, kdy, ka, kb, kz, kf, kh, kl, *keys = jax.random.split(jax.random.key(seed), 8 + 3 * len(NAMES))
    kx, kdy, ka, kb = (jax.random.fold_in(k, part) for k in (kx, kdy, ka, kb))
    kw, km, kv = (keys[i::3] for i in range(3))
    shape = (SEQUENCES, TOKENS, D)
    much_x, much_dy = jax.random.uniform(kz, (2,), jnp.float32, 0.0, 1.0)
    loud = 2.0 ** jax.random.uniform(jax.random.fold_in(kz, 1), (), jnp.float32, -1.0, 2.0)
    layers = 2.0 ** jax.random.uniform(kl, (LAYERS, 1, 1), jnp.float32, -1.0, 1.0)
    x = together(ka, jax.random.normal(kx, shape, jnp.float32), much_x) * bump(kf, D, 4.0)
    dy = together(kb, jax.random.normal(kdy, shape, jnp.float32), much_dy)
    drawn = {"x": x.astype(jnp.bfloat16), "dy": (loud * dy * (SEQUENCES * TOKENS) ** -0.5).astype(jnp.bfloat16)}
    for key, name in zip(kw, NAMES, strict=True):
        w = jax.random.normal(key, SHAPES[name], jnp.float32) * SHAPES[name][1] ** -0.5
        drawn[name] = (w * {"w_gate": 1.0, "w_up": bump(kh, FF, 4.0), "w_down": layers}[name]).astype(jnp.bfloat16)
    for key, name in zip(km, NAMES, strict=True):
        drawn[f"m_{name}"] = 0.1 * jax.random.normal(key, SHAPES[name], jnp.float32)
    for key, name in zip(kv, NAMES, strict=True):
        drawn[f"v_{name}"] = jax.random.uniform(key, SHAPES[name], jnp.float32, 0.005, 0.015)
    return drawn


def matmul(a, w):
    return jnp.dot(a, w, preferred_element_type=jnp.float32).astype(jnp.bfloat16)


def normed(h):
    wide = h.astype(jnp.float32)
    scale = lax.rsqrt(jnp.mean(wide**2, -1, keepdims=True) + 1e-6)
    return (wide * scale).astype(jnp.bfloat16)


def layer(h, w):
    a = normed(h)
    gate = jnp.dot(a, w["w_gate"], preferred_element_type=jnp.float32)
    up = jnp.dot(a, w["w_up"], preferred_element_type=jnp.float32)
    return h + matmul((jax.nn.silu(gate) * up).astype(jnp.bfloat16), w["w_down"])


def adamw(w, m, v, g):
    m = 0.9 * m + 0.1 * g
    v = 0.95 * v + 0.05 * g * g
    step = m * lax.rsqrt(v + 1e-8) + 0.1 * w
    return (w - 0.02 * step).astype(jnp.bfloat16), m, v


def clipped(gradients, sum_of_squares, count):
    factor = jnp.minimum(1.0, 0.5 * lax.rsqrt(sum_of_squares / count + 1e-30))
    return [g * factor for g in gradients]


def stack(weights, h):
    return lax.scan(lambda h, w: (layer(h, w), None), h, weights)[0]


def reference(x, dy, w_gate, w_up, w_down, m_w_gate, m_w_up, m_w_down, v_w_gate, v_w_up, v_w_down):
    weights = dict(zip(NAMES, (w_gate, w_up, w_down), strict=True))

    def take(so_far, sequence):
        h, by_y = sequence
        _, back = jax.vjp(lambda w: stack(w, h), weights)
        return jax.tree.map(lambda total, term: total + term.astype(jnp.float32), so_far, back(by_y)[0]), None

    none_yet = {name: jnp.zeros(w.shape, jnp.float32) for name, w in weights.items()}
    by_weights, _ = lax.scan(take, none_yet, (x, dy))
    gradients = [by_weights[name].astype(jnp.bfloat16).astype(jnp.float32) for name in NAMES]
    gradients = clipped(gradients, sum(jnp.sum(g * g) for g in gradients), sum(g.size for g in gradients))
    new = [
        adamw(w.astype(jnp.float32), m, v, g)
        for w, m, v, g in zip((w_gate, w_up, w_down), (m_w_gate, m_w_up, m_w_down), (v_w_gate, v_w_up, v_w_down), gradients, strict=True)
    ]
    return tuple(one[which] for which in range(3) for one in new)
```

```python
import functools
import types

import jax
import jax.numpy as jnp
from jax import lax
from jax.experimental import pallas as pl
from jax.experimental.pallas import tpu as pltpu
from jax.sharding import Mesh
from jax.sharding import PartitionSpec as P

bf16, f32 = jnp.bfloat16, jnp.float32
BY_AXES = pl.DeviceIdType.MESH
NN, NT, TN = ((1,), (0,)), ((1,), (1,)), ((0,), (0,))
UNIT = 256
PAIR = 2 * UNIT
PLANE = 4, 4
ALL = pl.ds(0, 4)
HALVES = pl.ds(0, 2), pl.ds(2, 2)
EPS = 1e-6


def dot(a, b, how):
    return lax.dot_general(a, b, (how, ((), ())), preferred_element_type=f32)


def sizes(x_shape, gate_shape, down_shape):
    s = types.SimpleNamespace()
    s.layers, s.rows, _ = gate_shape
    s.tokens, s.d = x_shape[1:]
    s.block = down_shape[1]
    s.padded = -(-s.block // 16) * 16
    s.ff = 16 * s.padded
    s.units = s.ff // UNIT
    s.sub = UNIT // 16
    s.early = -(-s.units // 2)
    s.late = s.units - s.early
    s.pair = 2 * s.rows
    s.both, s.wide, s.tile, s.half = 2 * s.tokens, 2 * s.ff, s.tokens // 4, s.d // 2
    return s


def here():
    return {name: lax.axis_index(name) for name in ("x", "y", "z", "c")}


def ring(v, k):
    return lax.rem(v + k + 4, 4)


def flip(v):
    return lax.rem(v, 2)


def greet(partners):
    barrier = pltpu.get_barrier_semaphore()
    for one in partners:
        pl.semaphore_signal(barrier, inc=1, device_id=one, device_id_type=BY_AXES)
    pl.semaphore_wait(barrier, len(partners))


def in_plane(me):
    return [{axis: ring(me[axis], k)} for axis in ("y", "z") for k in (1, -1)]


def beside(me):
    n = lax.axis_size("x")
    return [{"x": lax.rem(me["x"] + k, n)} for k in (1, n - 1)]


def twin(me):
    return {"c": 1 - me["c"]}


def remote(src, dst, sent, got, to):
    return pltpu.make_async_remote_copy(src_ref=src, dst_ref=dst, send_sem=sent, recv_sem=got, device_id=to, device_id_type=BY_AXES)


class Gather:
    def __init__(self, me, slot, sent, got, a, b):
        self.me, self.slot, self.sent, self.got, self.a, self.b = me, slot, sent, got, a, b

    def copy(self, u, m):
        i, j, x = self.me[self.a], self.me[self.b], self.me["x"]
        turn = 1 - 2 * flip(u)
        way = 1 - 2 * flip(u + x)
        came = ring(j, -way)
        if m < 2:
            at, to = (i, j), {self.a: ring(i, 1 - 2 * m)}
        elif m == 2:
            at, to = (ring(i, -turn), j), {self.a: ring(i, turn)}
        elif m == 3:
            at, to = (ALL, j), {self.b: ring(j, way)}
        elif m == 4:
            at, to = (ALL, came), {self.b: ring(j, way)}
        else:
            at, to = (pl.ds(2 * m - 10, 2), came), beside(self.me)[m - 5]
        ref = self.slot(u, *(at if self.a == "y" else at[::-1]))
        return remote(ref, ref, self.sent.at[u, m], self.got.at[u, m], to)

    def stage(self, k, u):
        for m in ((), (0, 1), (2,), (3,), (4, 5, 6))[k]:
            self.copy(u, m).wait_recv()
        for m in ((0, 1), (2,), (3,), (4, 5, 6), ())[k]:
            self.copy(u, m).start()
        if k == 4:
            for m in range(7):
                self.copy(u, m).wait_send()


def gather_sems(units):
    return [pltpu.SemaphoreType.DMA((units, 7)) for _ in range(8)]


DEPTH = 4


STAGES = 7


class Scatter:
    def __init__(self, me, bufs, sent, got, a, b):
        self.me, self.sent, self.got, self.a, self.b = me, sent, got, a, b
        self.term, self.rm, self.sm, self.r0, self.r1, self.t, self.q, self.s0, self.s1, self.x0, self.x1, self.tb, self.z0, self.z1 = bufs

    @staticmethod
    def scratch(rows, cols, units):
        sizes = [(3, 4, 4), (3, 4), (DEPTH,)] + [(2, 4)] * 4 + [(2,)] * 7
        return [pltpu.VMEM((*size, rows, cols), bf16) for size in sizes] + [pltpu.SemaphoreType.DMA((units, 11))] * 2

    def group(self, u, i, part=ALL):
        at = (i, part) if self.a == "y" else (part, i)
        return self.term.at[(lax.rem(u, 3), *at)]

    def copy(self, u, m):
        i, j, x = self.me[self.a], self.me[self.b], self.me["x"]
        turn, two, far = 1 - 2 * flip(u), flip(u), lax.rem(u, DEPTH)
        sems = self.sent.at[u, m], self.got.at[u, m]
        if m < 6:
            h, way = m % 2, 1 - 2 * (m % 2)
            same, other = HALVES[h], HALVES[1 - h]
            src, dst = ((self.group(u, ring(i, 2), same), self.r0.at[two, same]), (self.group(u, ring(i, way), other), self.rm.at[lax.rem(u, 3), other]), (self.t.at[two, same], self.r1.at[two, same]))[m // 2]
            return remote(src, dst, *sems, {self.a: ring(i, way)})
        if m < 9:
            src, dst, way = ((self.q.at[two, ring(j, 2)], self.s0.at[two], turn), (self.q.at[two, ring(j, -turn)], self.sm.at[far], -turn), (self.tb.at[two], self.s1.at[two], turn))[m - 6]
            return remote(src, dst, *sems, {self.b: ring(j, way)})
        src, dst = ((self.z0, self.x0), (self.z1, self.x1))[m - 9]
        way = (1 - 2 * flip(x)) * (1 if (self.a == "y") == (m == 9) else -1)
        return remote(src.at[two], dst.at[two], *sems, {"x": ring(x, way)})

    def start(self, u, m):
        for one in m:
            self.copy(u, one).start()

    def stage(self, k, u, put=None):
        i, j = self.me[self.a], self.me[self.b]
        turn, two, far = 1 - 2 * flip(u), flip(u), lax.rem(u, DEPTH)
        near, spread, last = range(6), range(6, 9), range(9, 11)
        for m in ((), near[:2], near[2:], spread[:1], spread[1:], last[:1], last[1:])[k]:
            self.copy(u, m).wait_recv()
        for m in ((), (), near, (), spread, last[:1], last[1:])[k]:
            self.copy(u, m).wait_send()
        wide = lambda ref, *at: ref[at].astype(f32)
        if k == 1:
            for half, way in zip(HALVES, (1, -1), strict=True):
                self.t[two, half] = (self.group(u, ring(i, way), half)[...].astype(f32) + wide(self.r0, two, half)).astype(bf16)
        if k == 2:
            self.q[two] = (self.group(u, i)[...].astype(f32) + wide(self.r1, two) + wide(self.rm, lax.rem(u, 3))).astype(bf16)
        if k == 3:
            self.tb[two] = (wide(self.q, two, ring(j, turn)) + wide(self.s0, two)).astype(bf16)
        if k == 4:
            self.z0[two] = (wide(self.q, two, j) + wide(self.s1, two) + wide(self.sm, far)).astype(bf16)
        if k == 5:
            self.z1[two] = (wide(self.z0, two) + wide(self.x0, two)).astype(bf16)
        if k == 6:
            put(u, wide(self.z1, two) + wide(self.x1, two))
        self.start(u, ((), near[4:], spread[:2], spread[2:], last[:1], last[1:], ())[k])


def call(kernel, name, number, **kw):
    params = dict(vmem_limit_bytes=67043328)
    if number is not None:
        params |= dict(collective_id=number, has_side_effects=True)
    return pl.pallas_call(kernel, name=name, compiler_params=pltpu.CompilerParams(**params), **kw)


ANY = pl.BlockSpec(memory_space=pl.ANY)


def whole(shape):
    return pl.BlockSpec(shape, lambda *_: (0,) * len(shape), pipeline_mode=pl.Buffered(1))


AXES = ("y", "z"), ("z", "y")
HALF = UNIT // 2


def streams_of(me, s, gates, downs, sems):
    out = []
    for buf, width in ((gates, UNIT), (downs, s.half)):
        for n, axes in enumerate(AXES):
            slot = lambda u, y, z, buf=buf, lanes=pl.ds(n * width, width): buf.at[u, y, z, :, lanes]
            out.append(Gather(me, slot, *sems[2 * len(out) : 2 * len(out) + 2], *axes))
    return out


def early(streams, units, stages):
    for k, u in stages:
        at_stage(streams, k, jnp.int32(u), units)


def at_stage(streams, k, u, units):
    @pl.when((u >= 0) & (u < units))
    def _():
        for stream in streams:
            stream.stage(k, u)


def silu_parts(gate):
    s = jax.nn.sigmoid(gate)
    return s, gate * s


def tiles(value, width, moves):
    lane = lax.broadcasted_iota(jnp.int32, (value.shape[0], HALF), 1)
    out = [jnp.zeros((value.shape[0], HALF), value.dtype)] * (width // HALF)
    for to, n, start in moves:
        for k in range(to // HALF, (to + n - 1) // HALF + 1):
            base = k * HALF - to
            low, high = max(start + base, 0), min(start + base + HALF, value.shape[1])
            piece = value[:, low:high]
            if high - low < HALF:
                gap = jnp.zeros((value.shape[0], HALF - (high - low)), value.dtype)
                piece = jnp.concatenate([gap, piece] if low > start + base else [piece, gap], 1)
            out[k] = jnp.where((lane >= -base) & (lane < n - base), piece, out[k])
    return out


def places(s, core):
    for u in range(s.units):
        for q in range(16):
            n = min(s.sub, s.block - u * s.sub)
            if n > 0:
                yield u * UNIT + q * s.sub, n, (2 * q + core) * s.block + u * s.sub


def prepare_kernel(s, wg, wu, wd, gates, downs, halves, padded, sems):
    me = here()
    greet([twin(me)])
    for layer in range(s.layers):
        for mat, w in enumerate((wg, wu)):
            for core in range(2):
                for k, tile in enumerate(tiles(w[layer].astype(f32), s.ff, places(s, core))):
                    halves[core, layer, k // 2, :, pl.ds(mat * UNIT + k % 2 * HALF, HALF)] = tile.astype(bf16)
        padded[layer] = jnp.concatenate([wd[:, layer], jnp.zeros((s.padded - s.block, s.d), bf16)], 0)
    c = me["c"]
    give = remote(halves.at[1 - c], gates.at[:, :, c], sems.at[0], sems.at[1], twin(me))
    keep = pltpu.make_async_copy(halves.at[c], gates.at[:, :, c], sems.at[2])
    rest = pltpu.make_async_copy(padded, downs, sems.at[3])
    for one in (give, keep, rest):
        one.start()
    for one in (give, keep, rest):
        one.wait()


VMEM = pl.BlockSpec(memory_space=pltpu.VMEM)


def array(*shape, dtype=bf16):
    return jax.ShapeDtypeStruct(shape, dtype)


def prepare(s, weights):
    half, down = (s.layers, s.units, s.rows, PAIR), (s.layers, s.padded, s.d)
    return call(
        functools.partial(prepare_kernel, s),
        "prepare",
        8,
        in_specs=[VMEM] * 3,
        out_specs=[ANY] * 2,
        out_shape=[array(s.layers, s.units, 2, s.rows, PAIR), array(*down)],
        scratch_shapes=[pltpu.VMEM((2, *half), bf16), pltpu.VMEM(down, bf16), pltpu.SemaphoreType.DMA((4,))],
    )(*weights)


WARM = [(k, d - k) for d in range(4) for k in range(d + 1)]


def parts(s):
    tile = s.tokens // 2
    return [pl.ds(n * tile, tile) for n in range(4)]


def lanes_of(u, width=UNIT):
    return pl.ds(pl.multiple_of(u * width, width), width)


def split(s, me, src, dst, u, width, sems):
    keep = pltpu.make_async_copy(src.at[pl.ds(0, s.tokens)], dst.at[:, lanes_of(u, width)], sems.at[0, u])
    give = remote(src.at[pl.ds(s.tokens, s.tokens)], dst.at[:, lanes_of(s.units + u, width)], sems.at[1, u], sems.at[2, u], twin(me))
    return keep, give


def first_kernel(s, x, dy, w, wd, acts, dys, gu, prod, downs, xv, av, pv, buf, dbuf, local, pair, prods, shared, *sems):
    me = here()
    j = pl.program_id(0)
    streams = streams_of(me, s, buf, dbuf, sems)
    y, z = me["y"], me["z"]
    rows = s.tile
    own_part = [pl.ds(n * rows, rows) for n in range(4)]

    def act_out(h):
        return pltpu.make_async_copy(av.at[pl.ds(h * s.tokens, s.tokens)], acts.at[h], local.at[5 + h])

    def share(n):
        return remote(av.at[own_part[n]], av.at[pl.ds(s.tokens + n * rows, rows)], pair.at[0, n], pair.at[1, n], twin(me))

    def prod_out(u):
        return split(s, me, pv.at[flip(u)], prod, u, UNIT, prods)

    def down_out(u):
        give = remote(dbuf.at[u], downs.at[1, u], shared.at[0, u], shared.at[1, u], twin(me))
        return pltpu.make_async_copy(dbuf.at[u], downs.at[0, u], shared.at[2, u]), give

    keep = pltpu.make_async_copy(xv.at[1], dys.at[0], local.at[4])
    give = remote(xv.at[1], dys.at[1], pair.at[0, 4], pair.at[1, 4], twin(me))

    @pl.when(j == 0)
    def _():
        own = [pltpu.make_async_copy(src.at[0], dst.at[:, y, z], local.at[n]) for n, (src, dst) in enumerate(((w, buf), (wd, dbuf)))]
        own += [pltpu.make_async_copy(one, xv.at[n], local.at[2 + n]) for n, one in enumerate((x, dy))]
        for one in own:
            one.start()
        greet(in_plane(me) + beside(me) + [twin(me)])
        own[0].wait()
        own[1].wait()
        early(streams, s.units, WARM[:3])
        own[2].wait()
        for n in range(4):
            wide = xv[0, own_part[n]].astype(f32)
            scale = lax.rsqrt(jnp.mean(wide * wide, -1, keepdims=True) + EPS)
            av[own_part[n]] = (wide * scale).astype(bf16)
            share(n).start()
            early(streams, s.units, WARM[3 + n : 4 + n])
        act_out(0).start()
        own[3].wait()
        keep.start()
        give.start()
        early(streams, s.units, WARM[7:])
        for n in range(4):
            share(n).wait()
        act_out(1).start()

    for k in range(5):
        at_stage(streams, 4 - k, j + k, s.units)
    for one in down_out(j):
        one.start()

    @pl.when(j >= 2)
    def _():
        for one in prod_out(j - 2):
            one.wait()

    weights = buf[j].reshape(s.d, PAIR)
    for part in parts(s):
        both = dot(av[part], weights, NN)
        gu[part] = both
        pv[flip(j), part] = (silu_parts(both[:, :UNIT])[1] * both[:, UNIT:]).astype(bf16)
    for one in prod_out(j):
        one.start()

    @pl.when(j == s.units - 1)
    def _():
        for one in (keep, give, act_out(0), act_out(1), *prod_out(j - 1), *prod_out(j)):
            one.wait()
        for u in range(s.units):
            for one in down_out(u):
                one.wait()


def first(s, x, dy, w, wd):
    both = (2, s.tokens, s.d)
    return call(
        functools.partial(first_kernel, s),
        "first",
        0,
        grid=(s.units,),
        in_specs=[ANY] * 4,
        out_specs=[ANY, ANY, pl.BlockSpec((s.both, PAIR), lambda j: (0, j)), ANY, ANY],
        out_shape=[array(*both), array(*both), array(s.both, s.wide, dtype=f32), array(s.tokens, s.wide), array(2, s.units, *PLANE, s.sub, s.d)],
        scratch_shapes=[
            pltpu.VMEM(both, bf16),
            pltpu.VMEM((s.both, s.d), bf16),
            pltpu.VMEM((2, s.both, UNIT), bf16),
            pltpu.VMEM((s.units, *PLANE, s.pair, PAIR), bf16),
            pltpu.VMEM((s.units, *PLANE, s.sub, s.d), bf16),
            pltpu.SemaphoreType.DMA((7,)),
            pltpu.SemaphoreType.DMA((2, 5)),
            pltpu.SemaphoreType.DMA((3, s.units)),
            pltpu.SemaphoreType.DMA((3, s.units)),
            *gather_sems(s.units),
        ],
    )(x, dy, w, wd)


class Both:
    def __init__(self, me, made, out, sems):
        self.me, self.made, self.out, self.sems = me, made, out, sems

    def copies(self, t):
        rows = self.made.shape[1]
        part, src = pl.ds(pl.multiple_of(t * rows, rows), rows), self.made.at[flip(t)]
        return pltpu.make_async_copy(src, self.out.at[0, part], self.sems.at[0, t]), remote(src, self.out.at[1, part], self.sems.at[1, t], self.sems.at[2, t], twin(self.me))

    def put(self, t, value):
        @pl.when(t >= 2)
        def _():
            for one in self.copies(t - 2):
                one.wait()

        self.made[flip(t)] = value
        for one in self.copies(t):
            one.start()

        @pl.when(t == 3)
        def _():
            for one in self.copies(t - 1) + self.copies(t):
                one.wait()


def tile_spec(s, width):
    return pl.BlockSpec((s.tile, width), lambda t: (t, 0))


def down_kernel(s, prod, w, h, wg, wd, h_out, acts, gates, downs, wv, total, gv, dv, local, saved, made, sent, *sems):
    me = here()
    t = pl.program_id(0)
    streams = streams_of(me, s, gv, dv, sems)
    loads = [pltpu.make_async_copy(w.at[n], wv.at[n], local.at[n]) for n in range(2)]

    @pl.when(t == 0)
    def _():
        y, z = me["y"], me["z"]
        own = [pltpu.make_async_copy(src.at[1, pl.ds(0, s.early)], dst.at[:, y, z], local.at[2 + n]) for n, (src, dst) in enumerate(((wg, gv), (wd, dv)))]
        for one in own + loads:
            one.start()
        greet(in_plane(me) + beside(me) + [twin(me)])
        for one in own:
            one.wait()

    def out(u):
        return [pltpu.make_async_copy(src.at[u], dst.at[u], saved.at[n, u]) for n, (src, dst) in enumerate(((gv, gates), (dv, downs)))]

    def slot(n):
        for k in reversed(range(5)):
            at_stage(streams, k, n - k, s.early)

        @pl.when((n >= 4) & (n < 4 + s.early))
        def _():
            for one in out(n - 4):
                one.start()

    slot(2 * t)

    @pl.when(t == 0)
    def _():
        loads[0].wait()

    total[...] = dot(prod[:, : s.ff], wv[0], NN)
    slot(2 * t + 1)

    @pl.when(t == 0)
    def _():
        loads[1].wait()

    y = (total[...] + dot(prod[:, s.ff :], wv[1], NN)).astype(bf16)
    new = (h[...].astype(f32) + y.astype(f32)).astype(bf16)
    h_out[...] = new
    wide = new.astype(f32)
    scale = lax.rsqrt(jnp.mean(wide * wide, -1, keepdims=True) + EPS)
    Both(me, made, acts, sent).put(t, (wide * scale).astype(bf16))

    @pl.when(t == 3)
    def _():
        slot(2 * t + 2)
        for u in range(s.early):
            for one in out(u):
                one.wait()


def own_rows(s):
    return [pltpu.VMEM((2, s.tile, s.d), bf16), pltpu.SemaphoreType.DMA((3, 4))]


def down(s, prod, w, h, wg, wd):
    tile = s.tile
    return call(
        functools.partial(down_kernel, s),
        "down",
        1,
        grid=(4,),
        in_specs=[tile_spec(s, s.wide), ANY, tile_spec(s, s.d), ANY, ANY],
        out_specs=[tile_spec(s, s.d), ANY, ANY, ANY],
        out_shape=[array(s.tokens, s.d), array(2, s.tokens, s.d), array(s.early, *PLANE, s.pair, PAIR), array(s.early, *PLANE, s.sub, s.d)],
        scratch_shapes=[
            pltpu.VMEM((2, s.ff, s.d), bf16),
            pltpu.VMEM((tile, s.d), f32),
            pltpu.VMEM((s.early, *PLANE, s.pair, PAIR), bf16),
            pltpu.VMEM((s.early, *PLANE, s.sub, s.d), bf16),
            pltpu.SemaphoreType.DMA((4,)),
            pltpu.SemaphoreType.DMA((2, s.early)),
            *own_rows(s),
            *gather_sems(s.early),
        ],
    )(prod, w, h, wg, wd)


def back_kernel(s, dgu, w0, w1, w2, h, by, out, wv, total, local, made, sent):
    me = here()
    t = pl.program_id(0)
    units = [w.at[u] for w in (w0, w1, w2) for u in range(w.shape[0])]
    loads = [pltpu.make_async_copy(one, wv.at[n // s.units, :, lanes_of(n % s.units, PAIR)], local.at[n]) for n, one in enumerate(units)]

    @pl.when(t == 0)
    def _():
        for load in loads:
            load.start()
        greet([twin(me)])
        for load in loads[: s.units]:
            load.wait()

    total[...] = dot(dgu[:, : s.wide], wv[0], NT)

    @pl.when(t == 0)
    def _():
        for load in loads[s.units :]:
            load.wait()

    da = (total[...] + dot(dgu[:, s.wide :], wv[1], NT)).astype(bf16).astype(f32)
    wide = h[...].astype(f32)
    scale = lax.rsqrt(jnp.mean(wide * wide, -1, keepdims=True) + EPS)
    along = jnp.mean(da * wide, -1, keepdims=True)
    dh = (scale * da - wide * (scale * scale * scale * along)).astype(bf16)
    Both(me, made, out, sent).put(t, (by[...].astype(f32) + dh.astype(f32)).astype(bf16))


def back(s, dgu, w0, w1, w2, h, by):
    return call(
        functools.partial(back_kernel, s),
        "back",
        2,
        grid=(4,),
        in_specs=[tile_spec(s, 2 * s.wide), ANY, ANY, ANY, tile_spec(s, s.d), tile_spec(s, s.d)],
        out_specs=ANY,
        out_shape=array(2, s.tokens, s.d),
        scratch_shapes=[pltpu.VMEM((2, s.d, s.wide), bf16), pltpu.VMEM((s.tile, s.d), f32), pltpu.SemaphoreType.DMA((2 * s.units,)), *own_rows(s)],
    )(dgu, w0, w1, w2, h, by)


def terms_scratch(s):
    return Scatter.scratch(s.pair, UNIT, s.units) * 2 + Scatter.scratch(s.sub, s.half, s.units) * 2


class Terms:
    def __init__(self, s, me, gates, downs, refs):
        self.s, self.gates, self.downs = s, gates, downs
        each = len(refs) // 4
        self.streams = [Scatter(me, refs[n * each : n * each + each - 2], *refs[n * each + each - 2 : n * each + each], *AXES[1 - n % 2]) for n in range(4)]

    def make(self, u, acts, dgu, prod, by):
        s, slot = self.s, lax.rem(u, 3)
        down = dot(prod[...], by[...], TN).astype(bf16)
        for n in range(2):
            self.streams[2 + n].term[slot] = down[:, n * s.half : (n + 1) * s.half].reshape(*PLANE, s.sub, s.half)
        for k in range(2):
            both = dot(acts[:, k * s.half : (k + 1) * s.half], dgu[...], TN).astype(bf16)
            for n in range(2):
                self.streams[n].term[slot, HALVES[k]] = both[:, n * UNIT : (n + 1) * UNIT].reshape(2, 4, s.pair, UNIT)

    def put(self, n, u, value):
        s = self.s
        if n < 2:
            self.gates[u, :, :, pl.ds(n * UNIT, UNIT)] = value.reshape(2, s.rows, UNIT).astype(bf16)
        else:
            self.downs[u, :, pl.ds((n - 2) * (s.half), s.half)] = value.astype(bf16)

    def settle(self, j):
        for k in reversed(range(STAGES)):
            u = j - k

            @pl.when((u >= 0) & (u < self.s.units))
            def _(k=k, u=u):
                for m in ((0, 1), (2, 3)) if k == 0 else ():
                    for stream in self.streams:
                        stream.start(u, m)
                for n, stream in enumerate(self.streams if k else ()):
                    stream.stage(k, u, functools.partial(self.put, n))


def sums(s):
    return [array(s.units, 2, s.rows, PAIR), array(s.units, s.sub, s.d)]


def arrivals(s, sources, targets, sems):
    return [[pltpu.make_async_copy(src.at[part], dst.at[part], sems.at[n, m]) for m, (src, dst) in enumerate(zip(sources, targets, strict=True))] for n, part in enumerate(parts(s))]


def wait_first(j, arrive):
    @pl.when(j == 0)
    def _():
        for one in sum(arrive, []):
            one.wait()


def back_gates(both, by):
    gate, up, by = both[:, :UNIT], both[:, UNIT:], by.astype(f32)
    sig, act = silu_parts(gate)
    return (by * up * (sig + act * (1.0 - sig))).astype(bf16), (by * act).astype(bf16), (act * up).astype(bf16)


def second_kernel(s, acts_in, dys_in, wg, wd, g_early, d_early, dgux, g_late, theirs, out_g, out_d, acts, dys, gv, dv, dgu, prod, tiles_in, local, saved, given, sent, *refs):
    me = here()
    j = pl.program_id(0)
    streams = streams_of(me, s, gv.at[pl.ds(2, s.late)], dv.at[pl.ds(2, s.late)], refs[:8])
    terms = Terms(s, me, out_g, out_d, refs[8:])

    def at(k, u):
        at_stage(streams, k, u, s.late)

    def load(u):
        return [pltpu.make_async_copy(src.at[u], dst.at[flip(u)], local.at[n, flip(u)]) for n, (src, dst) in enumerate(((g_early, gv), (d_early, dv)))]

    arrive = arrivals(s, (acts_in, dys_in), (acts, dys), tiles_in)

    def place(u):
        return jnp.where(u < s.early, flip(u), u - s.early + 2)

    def save(u):
        return pltpu.make_async_copy(gv.at[place(u)], g_late.at[u - s.early], saved)

    def give(u):
        return remote(gv.at[place(u)], theirs.at[u], given.at[0, u], given.at[1, u], twin(me))

    def dgu_out(u):
        return split(s, me, dgu, dgux, u, PAIR, sent)

    @pl.when(j == 0)
    def _():
        y, z = me["y"], me["z"]
        rest = pl.ds(s.early, s.late)
        own = [pltpu.make_async_copy(src.at[1, rest], dst.at[pl.ds(2, s.late), y, z], local.at[2, n]) for n, (src, dst) in enumerate(((wg, gv), (wd, dv)))]
        for one in own + load(0) + load(1) + sum(arrive, []):
            one.start()
        greet(in_plane(me) + beside(me) + [twin(me)])
        for one in own:
            one.wait()

    for k in reversed(range(5)):
        at(k, j - k)

    @pl.when((j >= 1) & (j <= s.units))
    def _():
        for one in (*dgu_out(j - 1), give(j - 1)):
            one.wait()

    @pl.when((j > s.early) & (j <= s.units))
    def _():
        save(j - 1).wait()

    @pl.when(j < s.units)
    def _():
        @pl.when(j < s.early)
        def _():
            for one in load(j):
                one.wait()

        @pl.when((j >= 1) & (j + 1 < s.early))
        def _():
            for one in load(j + 1):
                one.start()

        @pl.when(j >= s.early)
        def _():
            save(j).start()

        give(j).start()
        wait_first(j, arrive)
        now = place(j)
        weights, ahead = gv[now].reshape(s.d, PAIR), dv[now].reshape(UNIT, s.d)
        for part in parts(s):
            both = dot(acts[part], weights, NN)
            by = dot(dys[part], ahead, NT).astype(bf16)
            dgu[part, :UNIT], dgu[part, UNIT:], prod[part] = back_gates(both, by)
        for one in dgu_out(j):
            one.start()
        terms.make(j, acts, dgu, prod, dys)

    terms.settle(j)


def second(s, acts, dys, wg, wd, g_early, d_early):
    unit, row = (*PLANE, s.pair, PAIR), (*PLANE, s.sub, s.d)
    return call(
        functools.partial(second_kernel, s),
        "second",
        3,
        grid=(s.units + STAGES - 1,),
        in_specs=[ANY] * 6,
        out_specs=[ANY] * 3 + [whole(one.shape) for one in sums(s)],
        out_shape=[array(s.tokens, 2 * s.wide), array(s.late, *unit), array(s.units, *unit), *sums(s)],
        scratch_shapes=[
            *[pltpu.VMEM((s.both, s.d), bf16)] * 2,
            pltpu.VMEM((2 + s.late, *unit), bf16),
            pltpu.VMEM((2 + s.late, *row), bf16),
            pltpu.VMEM((s.both, PAIR), bf16),
            pltpu.VMEM((s.both, UNIT), bf16),
            pltpu.SemaphoreType.DMA((4, 2)),
            pltpu.SemaphoreType.DMA((3, 2)),
            pltpu.SemaphoreType.DMA,
            pltpu.SemaphoreType.DMA((2, s.units)),
            pltpu.SemaphoreType.DMA((3, s.units)),
            *gather_sems(s.late),
            *terms_scratch(s),
        ],
    )(acts, dys, wg, wd, g_early, d_early)


def third_kernel(s, acts_in, dh_in, wd, gu, out_g, out_d, acts, dh, dgu, prod, tiles_in, *refs):
    me = here()
    j = pl.program_id(0)
    terms = Terms(s, me, out_g, out_d, refs)
    arrive = arrivals(s, (dh_in, acts_in), (dh, acts), tiles_in)

    @pl.when(j == 0)
    def _():
        for one in sum(arrive, []):
            one.start()
        greet(in_plane(me) + beside(me))

    @pl.when(j < s.units)
    def _():
        wait_first(j, arrive)
        ahead = wd[...]
        for part in parts(s):
            by = dot(dh[part], ahead, NT).astype(bf16)
            dgu[part, :UNIT], dgu[part, UNIT:], prod[part] = back_gates(gu[part], by)
        terms.make(j, acts, dgu, prod, dh)

    terms.settle(j)


def third(s, number, acts, dh, wd, gu):
    at = lambda j: jnp.minimum(j, s.units - 1)
    return call(
        functools.partial(third_kernel, s),
        "third",
        number,
        grid=(s.units + STAGES - 1,),
        in_specs=[ANY] * 2 + [pl.BlockSpec((UNIT, s.d), lambda j: (at(j), 0)), pl.BlockSpec((s.both, PAIR), lambda j: (0, at(j)))],
        out_specs=[whole(one.shape) for one in sums(s)],
        out_shape=sums(s),
        scratch_shapes=[
            *[pltpu.VMEM((s.both, s.d), bf16)] * 2,
            pltpu.VMEM((s.both, PAIR), bf16),
            pltpu.VMEM((s.both, UNIT), bf16),
            pltpu.SemaphoreType.DMA((4, 2)),
            *terms_scratch(s),
        ],
    )(acts, dh, wd, gu)


def adamw(w, m, v, g):
    m = 0.9 * m + 0.1 * g
    v = 0.95 * v + 0.05 * g * g
    step = m * lax.rsqrt(v + 1e-8) + 0.1 * w
    return (w - 0.02 * step).astype(bf16), m, v


def total_kernel(g0, d0, g1, d1, got, out, sums, sent, here_got):
    me = here()
    greet(in_plane(me) + [{axis: ring(me[axis], 2)} for axis in ("y", "z")] + [twin(me)])
    pairs = [remote(g.at[:, 1 - me["c"]], got.at[n], sent.at[n], here_got.at[n], twin(me)) for n, g in enumerate((g0, g1))]
    for one in pairs:
        one.start()
    total = sum(jnp.sum(g[...].astype(f32) ** 2) for g in (g0, d0, g1, d1))
    total = jnp.full(out.shape, total)
    base = 0
    for axis in "cyz":
        size = lax.axis_size(axis)
        sums[base] = total
        copies = []
        for k in range(1, size):
            to = {axis: lax.rem(me[axis] + k, size)}
            copies.append(remote(sums.at[base], sums.at[base + k], sent.at[base + k + 1], here_got.at[base + k + 1], to))
            copies[-1].start()
        for k, one in enumerate(copies):
            one.wait()
            total += sums[base + k + 1]
        base += size
    out[...] = total
    for one in pairs:
        one.wait()


def total(number, *sums):
    tile, shape = (8, HALF), sums[0].shape
    sems = pltpu.SemaphoreType.DMA((12,))
    return call(
        total_kernel,
        "total",
        number,
        in_specs=[VMEM] * 4,
        out_specs=[VMEM] * 2,
        out_shape=[array(2, shape[0], *shape[2:]), array(*tile, dtype=f32)],
        scratch_shapes=[pltpu.VMEM((10, *tile), f32), sems, sems],
    )(*sums)


def finish_kernel(s, g0, d0, g1, d1, got, squares, *refs):
    old, new = refs[:9], refs[9:]
    c = lax.axis_index("c")
    count = 16 * (s.layers * s.pair * 32 * s.block * 3)
    factor = jnp.minimum(1.0, 0.5 * lax.rsqrt(squares[:1, :1] / count + 1e-30))
    moves = [(start, n, core * s.ff + to) for core in range(2) for to, n, start in places(s, core)]

    def update(n, at, g):
        w, m, v = (old[n + 3 * k] for k in range(3))
        made = adamw(w[at].astype(f32), m[at], v[at], g * factor)
        for k, value in enumerate(made):
            new[n + 3 * k][at] = value

    for layer, (g, d) in enumerate(((g0, d0), (g1, d1))):
        for mat in range(2):
            lanes = pl.ds(mat * UNIT, UNIT)
            pieces = [[ref[u, c, :, lanes] if ref is g else ref[layer, u, :, lanes] for u in range(s.units)] for ref in (g, got)]
            mine, other = (jnp.concatenate(piece, 1).astype(f32) for piece in pieces)
            both = jnp.concatenate([jnp.where(c == 0, mine, other), jnp.where(c == 0, other, mine)], 1)
            update(mat, layer, jnp.concatenate(tiles(both, 32 * s.block, moves), 1))
        update(2, (slice(None), layer), d[...].astype(f32).reshape(s.padded, s.d)[: s.block])


def finish(s, sums, got, squares, old):
    out = [array(*one.shape, dtype=one.dtype) for one in old]
    return call(functools.partial(finish_kernel, s), "finish", None, in_specs=[VMEM] * 15, out_specs=[VMEM] * 9, out_shape=out)(*sums, got, squares, *old)


def turned(arrays):
    return [one.swapaxes(0, 1) if n % 3 == 2 else one for n, one in enumerate(arrays)]


def solution(mesh):
    cut_mesh = Mesh(mesh.devices.reshape(mesh.shape["rep"], mesh.shape["r"], 4, 4, 2), ("rep", "x", "y", "z", "c"))

    def step(x, dy, *arrays):
        s = sizes(x.shape, arrays[0].shape, arrays[2].shape)
        arrays = turned(arrays)
        flat = (s.both, s.d)
        gates, downs = prepare(s, arrays[:3])
        gates = gates.reshape(s.layers, s.units, s.pair, PAIR)
        downs = downs.reshape(s.layers, s.units, s.sub, s.d)
        acts0, dys, gu0, prod0, wd0 = first(s, x[0], dy[0], gates, downs)
        h1, acts1, g_early, d_early = down(s, prod0, wd0.reshape(2, s.ff, s.d), x[0], gates, downs)
        dys, acts0, acts1 = (one.reshape(flat) for one in (dys, acts0, acts1))
        dgu1, g_late, theirs, *sums1 = second(s, acts1, dys, gates, downs, g_early, d_early)
        w = (one.reshape(-1, s.d, PAIR) for one in (g_early, g_late, theirs))
        dh = back(s, dgu1, *w, h1, dy[0]).reshape(flat)
        sums0 = third(s, 6, acts0, dh, wd0.reshape(-1, s.d), gu0)
        return tuple(turned(finish(s, (*sums0, *sums1), *total(7, *sums0, *sums1), arrays)))

    place = ("y", "z", "c")
    states, cut = P(("rep", "x", *place), None, None), P(None, place, None)
    return jax.shard_map(
        step,
        mesh=cut_mesh,
        in_specs=(states, states) + (cut,) * 9,
        out_specs=(P("rep", place, None),) * 9,
        check_vma=False,
    )
```

```python
import functools
import types

import jax
import jax.numpy as jnp
from jax import lax
from jax.experimental import pallas as pl
from jax.experimental.pallas import tpu as pltpu
from jax.sharding import Mesh
from jax.sharding import PartitionSpec as P

bf16, f32 = jnp.bfloat16, jnp.float32
BY_AXES = pl.DeviceIdType.MESH
NN, NT, TN = ((1,), (0,)), ((1,), (1,)), ((0,), (0,))
UNIT = 256
PAIR = 2 * UNIT
PLANE = 4, 4
TILES = 8
ALL = pl.ds(0, 4)
HALVES = pl.ds(0, 2), pl.ds(2, 2)
EPS = 1e-6


def dot(a, b, how):
    return lax.dot_general(a, b, (how, ((), ())), preferred_element_type=f32)


def sizes(x_shape, gate_shape, down_shape):
    s = types.SimpleNamespace()
    s.layers, s.rows, _ = gate_shape
    s.tokens, s.d = x_shape[1:]
    s.block = down_shape[1]
    s.padded = -(-s.block // 16) * 16
    s.ff = 16 * s.padded
    s.units = s.ff // UNIT
    s.sub = UNIT // 16
    s.early = s.units // 3
    s.late = s.units - s.early
    s.pair = 2 * s.rows
    s.both, s.wide, s.tile, s.half = 2 * s.tokens, 2 * s.ff, s.tokens // TILES, s.d // 2
    return s


def here():
    return {name: lax.axis_index(name) for name in ("x", "y", "z", "c")}


def ring(v, k):
    return lax.rem(v + k + 4, 4)


def flip(v):
    return lax.rem(v, 2)


def greet(partners):
    barrier = pltpu.get_barrier_semaphore()
    for one in partners:
        pl.semaphore_signal(barrier, inc=1, device_id=one, device_id_type=BY_AXES)
    pl.semaphore_wait(barrier, len(partners))


def in_plane(me):
    return [{axis: ring(me[axis], k)} for axis in ("y", "z") for k in (1, -1)]


def beside(me):
    n = lax.axis_size("x")
    return [{"x": lax.rem(me["x"] + k, n)} for k in (1, n - 1)]


def twin(me):
    return {"c": 1 - me["c"]}


def remote(src, dst, sent, got, to):
    return pltpu.make_async_remote_copy(src_ref=src, dst_ref=dst, send_sem=sent, recv_sem=got, device_id=to, device_id_type=BY_AXES)


class Gather:
    def __init__(self, me, slot, sent, got, a, b):
        self.me, self.slot, self.sent, self.got, self.a, self.b = me, slot, sent, got, a, b

    def copy(self, u, m):
        i, j, x = self.me[self.a], self.me[self.b], self.me["x"]
        turn = 1 - 2 * flip(u)
        way = 1 - 2 * flip(u + x)
        came = ring(j, -way)
        if m < 2:
            at, to = (i, j), {self.a: ring(i, 1 - 2 * m)}
        elif m == 2:
            at, to = (ring(i, -turn), j), {self.a: ring(i, turn)}
        elif m == 3:
            at, to = (ALL, j), {self.b: ring(j, way)}
        elif m == 4:
            at, to = (ALL, came), {self.b: ring(j, way)}
        else:
            at, to = (pl.ds(2 * m - 10, 2), came), beside(self.me)[m - 5]
        ref = self.slot(u, *(at if self.a == "y" else at[::-1]))
        return remote(ref, ref, self.sent.at[u, m], self.got.at[u, m], to)

    def stage(self, k, u):
        for m in ((), (0, 1), (2,), (3,), (4, 5, 6))[k]:
            self.copy(u, m).wait_recv()
        for m in ((0, 1), (2,), (3,), (4, 5, 6), ())[k]:
            self.copy(u, m).start()
        if k == 4:
            for m in range(7):
                self.copy(u, m).wait_send()


def gather_sems(units):
    return [pltpu.SemaphoreType.DMA((units, 7)) for _ in range(8)]


DEPTH = 4


STAGES = 7


class Scatter:
    def __init__(self, me, bufs, sent, got, a, b):
        self.me, self.sent, self.got, self.a, self.b = me, sent, got, a, b
        self.term, self.rm, self.sm, self.r0, self.r1, self.t, self.q, self.s0, self.s1, self.x0, self.x1, self.tb, self.z0, self.z1 = bufs

    @staticmethod
    def scratch(rows, cols, units):
        sizes = [(3, 4, 4), (3, 4), (DEPTH,)] + [(2, 4)] * 4 + [(2,)] * 7
        return [pltpu.VMEM((*size, rows, cols), bf16) for size in sizes] + [pltpu.SemaphoreType.DMA((units, 11))] * 2

    def group(self, u, i, part=ALL):
        at = (i, part) if self.a == "y" else (part, i)
        return self.term.at[(lax.rem(u, 3), *at)]

    def copy(self, u, m):
        i, j, x = self.me[self.a], self.me[self.b], self.me["x"]
        turn, two, far = 1 - 2 * flip(u), flip(u), lax.rem(u, DEPTH)
        sems = self.sent.at[u, m], self.got.at[u, m]
        if m < 6:
            h, way = m % 2, 1 - 2 * (m % 2)
            same, other = HALVES[h], HALVES[1 - h]
            src, dst = ((self.group(u, ring(i, 2), same), self.r0.at[two, same]), (self.group(u, ring(i, way), other), self.rm.at[lax.rem(u, 3), other]), (self.t.at[two, same], self.r1.at[two, same]))[m // 2]
            return remote(src, dst, *sems, {self.a: ring(i, way)})
        if m < 9:
            src, dst, way = ((self.q.at[two, ring(j, 2)], self.s0.at[two], turn), (self.q.at[two, ring(j, -turn)], self.sm.at[far], -turn), (self.tb.at[two], self.s1.at[two], turn))[m - 6]
            return remote(src, dst, *sems, {self.b: ring(j, way)})
        src, dst = ((self.z0, self.x0), (self.z1, self.x1))[m - 9]
        way = (1 - 2 * flip(x)) * (1 if (self.a == "y") == (m == 9) else -1)
        return remote(src.at[two], dst.at[two], *sems, {"x": ring(x, way)})

    def start(self, u, m):
        for one in m:
            self.copy(u, one).start()

    def stage(self, k, u, put=None):
        i, j = self.me[self.a], self.me[self.b]
        turn, two, far = 1 - 2 * flip(u), flip(u), lax.rem(u, DEPTH)
        near, spread, last = range(6), range(6, 9), range(9, 11)
        for m in ((), near[:2], near[2:], spread[:1], spread[1:], last[:1], last[1:])[k]:
            self.copy(u, m).wait_recv()
        for m in ((), (), near, (), spread, last[:1], last[1:])[k]:
            self.copy(u, m).wait_send()
        wide = lambda ref, *at: ref[at].astype(f32)
        if k == 1:
            for half, way in zip(HALVES, (1, -1), strict=True):
                self.t[two, half] = (self.group(u, ring(i, way), half)[...].astype(f32) + wide(self.r0, two, half)).astype(bf16)
        if k == 2:
            self.q[two] = (self.group(u, i)[...].astype(f32) + wide(self.r1, two) + wide(self.rm, lax.rem(u, 3))).astype(bf16)
        if k == 3:
            self.tb[two] = (wide(self.q, two, ring(j, turn)) + wide(self.s0, two)).astype(bf16)
        if k == 4:
            self.z0[two] = (wide(self.q, two, j) + wide(self.s1, two) + wide(self.sm, far)).astype(bf16)
        if k == 5:
            self.z1[two] = (wide(self.z0, two) + wide(self.x0, two)).astype(bf16)
        if k == 6:
            put(u, wide(self.z1, two) + wide(self.x1, two))
        self.start(u, ((), near[4:], spread[:2], spread[2:], last[:1], last[1:], ())[k])


def call(kernel, name, number, **kw):
    params = dict(vmem_limit_bytes=67043328)
    if number is not None:
        params |= dict(collective_id=number, has_side_effects=True)
    return pl.pallas_call(kernel, name=name, compiler_params=pltpu.CompilerParams(**params), **kw)


ANY = pl.BlockSpec(memory_space=pl.ANY)


def whole(shape):
    return pl.BlockSpec(shape, lambda *_: (0,) * len(shape), pipeline_mode=pl.Buffered(1))


AXES = ("y", "z"), ("z", "y")
HALF = UNIT // 2


def streams_of(me, s, gates, downs, sems):
    out = []
    for buf, width in ((gates, UNIT), (downs, s.half)):
        for n, axes in enumerate(AXES):
            slot = lambda u, y, z, buf=buf, lanes=pl.ds(n * width, width): buf.at[u, y, z, :, lanes]
            out.append(Gather(me, slot, *sems[2 * len(out) : 2 * len(out) + 2], *axes))
    return out


def early(streams, units, stages):
    for k, u in stages:
        at_stage(streams, k, jnp.int32(u), units)


def at_stage(streams, k, u, units):
    @pl.when((u >= 0) & (u < units))
    def _():
        for stream in streams:
            stream.stage(k, u)


def silu_parts(gate):
    s = jax.nn.sigmoid(gate)
    return s, gate * s


def tiles(value, width, moves):
    lane = lax.broadcasted_iota(jnp.int32, (value.shape[0], HALF), 1)
    out = [jnp.zeros((value.shape[0], HALF), value.dtype)] * (width // HALF)
    for to, n, start in moves:
        for k in range(to // HALF, (to + n - 1) // HALF + 1):
            base = k * HALF - to
            low, high = max(start + base, 0), min(start + base + HALF, value.shape[1])
            piece = value[:, low:high]
            if high - low < HALF:
                gap = jnp.zeros((value.shape[0], HALF - (high - low)), value.dtype)
                piece = jnp.concatenate([gap, piece] if low > start + base else [piece, gap], 1)
            out[k] = jnp.where((lane >= -base) & (lane < n - base), piece, out[k])
    return out


def places(s, core):
    for u in range(s.units):
        for q in range(16):
            n = min(s.sub, s.block - u * s.sub)
            if n > 0:
                yield u * UNIT + q * s.sub, n, (2 * q + core) * s.block + u * s.sub


def prepare_kernel(s, wg, wu, wd, gates, downs, halves, padded, sems):
    me = here()
    greet([twin(me)])
    for layer in range(s.layers):
        for mat, w in enumerate((wg, wu)):
            for core in range(2):
                for k, tile in enumerate(tiles(w[layer].astype(f32), s.ff, places(s, core))):
                    halves[core, layer, k // 2, :, pl.ds(mat * UNIT + k % 2 * HALF, HALF)] = tile.astype(bf16)
        padded[layer] = jnp.concatenate([wd[:, layer], jnp.zeros((s.padded - s.block, s.d), bf16)], 0)
    c = me["c"]
    give = remote(halves.at[1 - c], gates.at[:, :, c], sems.at[0], sems.at[1], twin(me))
    keep = pltpu.make_async_copy(halves.at[c], gates.at[:, :, c], sems.at[2])
    rest = pltpu.make_async_copy(padded, downs, sems.at[3])
    for one in (give, keep, rest):
        one.start()
    for one in (give, keep, rest):
        one.wait()


VMEM = pl.BlockSpec(memory_space=pltpu.VMEM)


def array(*shape, dtype=bf16):
    return jax.ShapeDtypeStruct(shape, dtype)


def prepare(s, weights):
    half, down = (s.layers, s.units, s.rows, PAIR), (s.layers, s.padded, s.d)
    return call(
        functools.partial(prepare_kernel, s),
        "prepare",
        8,
        in_specs=[VMEM] * 3,
        out_specs=[ANY] * 2,
        out_shape=[array(s.layers, s.units, 2, s.rows, PAIR), array(*down)],
        scratch_shapes=[pltpu.VMEM((2, *half), bf16), pltpu.VMEM(down, bf16), pltpu.SemaphoreType.DMA((4,))],
    )(*weights)


WARM = [(k, d - k) for d in range(4) for k in range(d + 1)]


def parts(s):
    tile = s.tokens // 2
    return [pl.ds(n * tile, tile) for n in range(4)]


def lanes_of(u, width=UNIT):
    return pl.ds(pl.multiple_of(u * width, width), width)


def split(s, me, src, dst, u, width, sems):
    keep = pltpu.make_async_copy(src.at[pl.ds(0, s.tokens)], dst.at[:, lanes_of(u, width)], sems.at[0, u])
    give = remote(src.at[pl.ds(s.tokens, s.tokens)], dst.at[:, lanes_of(s.units + u, width)], sems.at[1, u], sems.at[2, u], twin(me))
    return keep, give


def first_kernel(s, x, dy, w, wd, acts, dys, gu, prod, downs, xv, av, pv, buf, dbuf, local, pair, prods, shared, *sems):
    me = here()
    j = pl.program_id(0)
    streams = streams_of(me, s, buf, dbuf, sems)
    y, z = me["y"], me["z"]
    rows = s.tokens // 4
    own_part = [pl.ds(n * rows, rows) for n in range(4)]

    def act_out(h):
        return pltpu.make_async_copy(av.at[pl.ds(h * s.tokens, s.tokens)], acts.at[h], local.at[5 + h])

    def share(n):
        return remote(av.at[own_part[n]], av.at[pl.ds(s.tokens + n * rows, rows)], pair.at[0, n], pair.at[1, n], twin(me))

    def prod_out(u):
        return split(s, me, pv.at[flip(u)], prod, u, UNIT, prods)

    def down_out(u):
        give = remote(dbuf.at[u], downs.at[1, u], shared.at[0, u], shared.at[1, u], twin(me))
        return pltpu.make_async_copy(dbuf.at[u], downs.at[0, u], shared.at[2, u]), give

    keep = pltpu.make_async_copy(xv.at[1], dys.at[0], local.at[4])
    give = remote(xv.at[1], dys.at[1], pair.at[0, 4], pair.at[1, 4], twin(me))

    @pl.when(j == 0)
    def _():
        own = [pltpu.make_async_copy(src.at[0], dst.at[:, y, z], local.at[n]) for n, (src, dst) in enumerate(((w, buf), (wd, dbuf)))]
        own += [pltpu.make_async_copy(one, xv.at[n], local.at[2 + n]) for n, one in enumerate((x, dy))]
        for one in own:
            one.start()
        greet(in_plane(me) + beside(me) + [twin(me)])
        own[0].wait()
        own[1].wait()
        early(streams, s.units, WARM[:3])
        own[2].wait()
        for n in range(4):
            wide = xv[0, own_part[n]].astype(f32)
            scale = lax.rsqrt(jnp.mean(wide * wide, -1, keepdims=True) + EPS)
            av[own_part[n]] = (wide * scale).astype(bf16)
            share(n).start()
            early(streams, s.units, WARM[3 + n : 4 + n])
        act_out(0).start()
        own[3].wait()
        keep.start()
        give.start()
        early(streams, s.units, WARM[7:])
        for n in range(4):
            share(n).wait()
        act_out(1).start()

    for k in range(5):
        at_stage(streams, 4 - k, j + k, s.units)
    for one in down_out(j):
        one.start()

    @pl.when(j >= 2)
    def _():
        for one in prod_out(j - 2):
            one.wait()

    weights = buf[j].reshape(s.d, PAIR)
    for part in parts(s):
        both = dot(av[part], weights, NN)
        gu[part] = both
        pv[flip(j), part] = (silu_parts(both[:, :UNIT])[1] * both[:, UNIT:]).astype(bf16)
    for one in prod_out(j):
        one.start()

    @pl.when(j == s.units - 1)
    def _():
        for one in (keep, give, act_out(0), act_out(1), *prod_out(j - 1), *prod_out(j)):
            one.wait()
        for u in range(s.units):
            for one in down_out(u):
                one.wait()


def first(s, x, dy, w, wd):
    both = (2, s.tokens, s.d)
    return call(
        functools.partial(first_kernel, s),
        "first",
        0,
        grid=(s.units,),
        in_specs=[ANY] * 4,
        out_specs=[ANY, ANY, pl.BlockSpec((s.both, PAIR), lambda j: (0, j)), ANY, ANY],
        out_shape=[array(*both), array(*both), array(s.both, s.wide, dtype=f32), array(s.tokens, s.wide), array(2, s.units, *PLANE, s.sub, s.d)],
        scratch_shapes=[
            pltpu.VMEM(both, bf16),
            pltpu.VMEM((s.both, s.d), bf16),
            pltpu.VMEM((2, s.both, UNIT), bf16),
            pltpu.VMEM((s.units, *PLANE, s.pair, PAIR), bf16),
            pltpu.VMEM((s.units, *PLANE, s.sub, s.d), bf16),
            pltpu.SemaphoreType.DMA((7,)),
            pltpu.SemaphoreType.DMA((2, 5)),
            pltpu.SemaphoreType.DMA((3, s.units)),
            pltpu.SemaphoreType.DMA((3, s.units)),
            *gather_sems(s.units),
        ],
    )(x, dy, w, wd)


class Both:
    def __init__(self, s, me, out, total, made, sems):
        self.s, self.me, self.out, self.total, self.made, self.sems = s, me, out, total, made, sems

    @staticmethod
    def scratch(s):
        return [pltpu.VMEM((s.tile, s.d), f32), pltpu.VMEM((2, s.tile, s.d), bf16), pltpu.SemaphoreType.DMA((3, TILES))]

    def copies(self, t):
        part, src = pl.ds(pl.multiple_of(t * self.s.tile, self.s.tile), self.s.tile), self.made.at[flip(t)]
        keep = pltpu.make_async_copy(src, self.out.at[0, part], self.sems.at[0, t])
        return keep, remote(src, self.out.at[1, part], self.sems.at[1, t], self.sems.at[2, t], twin(self.me))

    def step(self, t, product, make):
        @pl.when(t > 2)
        def _():
            for one in self.copies(t - 3):
                one.wait()

        def finish():
            self.made[flip(t - 1)] = make(self.total[...])
            for one in self.copies(t - 1):
                one.start()

        @pl.when((t > 0) & (t < TILES))
        def _():
            finish()
            self.total[...] = product()

        @pl.when(t == TILES)
        def _():
            finish()
            for one in self.copies(t - 2) + self.copies(t - 1):
                one.wait()


def tile_spec(s, width, late):
    return pl.BlockSpec((s.tile, width), lambda t: (jnp.clip(t - late, 0, TILES - 1), 0))


def down_kernel(s, prod, w, h, wg, wd, h_out, acts, gates, downs, wv, gv, dv, local, saved, *refs):
    me = here()
    t = pl.program_id(0)
    both, streams = Both(s, me, acts, *refs[:3]), streams_of(me, s, gv, dv, refs[3:])
    thirds = [pl.ds(n * s.wide // 3, s.wide // 3) for n in range(3)]

    def out(u):
        return [pltpu.make_async_copy(src.at[u], dst.at[u], saved.at[n, u]) for n, (src, dst) in enumerate(((gv, gates), (dv, downs)))]

    def slot(n):
        for k in reversed(range(5)):
            at_stage(streams, k, n - 2 * k, s.early)

        @pl.when((n >= TILES) & (n < TILES + s.early))
        def _():
            for one in out(n - TILES):
                one.start()

    @pl.when(t == 0)
    def _():
        loads = [pltpu.make_async_copy(w.at[part], wv.at[part], local.at[n]) for n, part in enumerate(thirds)]
        own = [pltpu.make_async_copy(src.at[1, pl.ds(0, s.early)], dst.at[:, me["y"], me["z"]], local.at[3 + n]) for n, (src, dst) in enumerate(((wg, gv), (wd, dv)))]
        for one in own + loads:
            one.start()
        greet(in_plane(me) + beside(me) + [twin(me)])
        for one in own:
            one.wait()
        for n, part in enumerate(thirds):
            slot(jnp.int32(n))
            loads[n].wait()
            product = dot(prod[:, part], wv[part], NN)
            both.total[...] = both.total[...] + product if n else product

    @pl.when(t > 0)
    def _():
        slot(t + 2)

    def make(total):
        new = (h[...].astype(f32) + total.astype(bf16).astype(f32)).astype(bf16)
        h_out[...] = new
        wide = new.astype(f32)
        scale = lax.rsqrt(jnp.mean(wide * wide, -1, keepdims=True) + EPS)
        return (wide * scale).astype(bf16)

    both.step(t, lambda: dot(prod[...], wv[...], NN), make)

    @pl.when(t == TILES)
    def _():
        for u in range(s.early):
            for one in out(u):
                one.wait()


def down(s, prod, w, h, wg, wd):
    unit, row = (s.early, *PLANE, s.pair, PAIR), (s.early, *PLANE, s.sub, s.d)
    return call(
        functools.partial(down_kernel, s),
        "down",
        1,
        grid=(TILES + 1,),
        in_specs=[tile_spec(s, s.wide, 0), ANY, tile_spec(s, s.d, 1), ANY, ANY],
        out_specs=[tile_spec(s, s.d, 1), ANY, ANY, ANY],
        out_shape=[array(s.tokens, s.d), array(2, s.tokens, s.d), array(*unit), array(*row)],
        scratch_shapes=[
            pltpu.VMEM((s.wide, s.d), bf16),
            pltpu.VMEM(unit, bf16),
            pltpu.VMEM(row, bf16),
            pltpu.SemaphoreType.DMA((5,)),
            pltpu.SemaphoreType.DMA((2, s.early)),
            *Both.scratch(s),
            *gather_sems(s.early),
        ],
    )(prod, w, h, wg, wd)


def back_kernel(s, dgu, w0, w1, w2, h, by, out, wv, local, *refs):
    me = here()
    t = pl.program_id(0)
    both = Both(s, me, out, *refs)
    units = [w.at[u] for w in (w0, w1, w2) for u in range(w.shape[0])]

    @pl.when(t == 0)
    def _():
        loads = [pltpu.make_async_copy(one, wv.at[:, pl.ds(n * PAIR, PAIR)], local.at[n]) for n, one in enumerate(units)]
        for load in loads:
            load.start()
        greet([twin(me)])
        each = len(units) // 3
        for n in range(3):
            for load in loads[n * each : (n + 1) * each]:
                load.wait()
            part = pl.ds(n * each * PAIR, each * PAIR)
            product = dot(dgu[:, part], wv[:, part], NT)
            both.total[...] = both.total[...] + product if n else product

    def make(total):
        da = total.astype(bf16).astype(f32)
        wide = h[...].astype(f32)
        scale = lax.rsqrt(jnp.mean(wide * wide, -1, keepdims=True) + EPS)
        along = jnp.mean(da * wide, -1, keepdims=True)
        dh = (scale * da - wide * (scale * scale * scale * along)).astype(bf16)
        return (by[...].astype(f32) + dh.astype(f32)).astype(bf16)

    both.step(t, lambda: dot(dgu[...], wv[...], NT), make)


def back(s, dgu, w0, w1, w2, h, by):
    return call(
        functools.partial(back_kernel, s),
        "back",
        2,
        grid=(TILES + 1,),
        in_specs=[tile_spec(s, 2 * s.wide, 0), ANY, ANY, ANY, tile_spec(s, s.d, 1), tile_spec(s, s.d, 1)],
        out_specs=ANY,
        out_shape=array(2, s.tokens, s.d),
        scratch_shapes=[pltpu.VMEM((s.d, 2 * s.wide), bf16), pltpu.SemaphoreType.DMA((2 * s.units,)), *Both.scratch(s)],
    )(dgu, w0, w1, w2, h, by)


def terms_scratch(s):
    return Scatter.scratch(s.pair, UNIT, s.units) * 2 + Scatter.scratch(s.sub, s.half, s.units) * 2


class Terms:
    def __init__(self, s, me, gates, downs, refs):
        self.s, self.gates, self.downs = s, gates, downs
        each = len(refs) // 4
        self.streams = [Scatter(me, refs[n * each : n * each + each - 2], *refs[n * each + each - 2 : n * each + each], *AXES[1 - n % 2]) for n in range(4)]

    def make(self, u, acts, dgu, prod, by, between=()):
        s, slot = self.s, lax.rem(u, 3)
        down = dot(prod[...], by[...], TN).astype(bf16)
        for n in range(2):
            self.streams[2 + n].term[slot] = down[:, n * s.half : (n + 1) * s.half].reshape(*PLANE, s.sub, s.half)
        for one in between:
            one.start()
        for k in range(2):
            both = dot(acts[:, k * s.half : (k + 1) * s.half], dgu[...], TN).astype(bf16)
            for n in range(2):
                self.streams[n].term[slot, HALVES[k]] = both[:, n * UNIT : (n + 1) * UNIT].reshape(2, 4, s.pair, UNIT)

    def put(self, n, u, value):
        s = self.s
        if n < 2:
            self.gates[u, :, :, pl.ds(n * UNIT, UNIT)] = value.reshape(2, s.rows, UNIT).astype(bf16)
        else:
            self.downs[u, :, pl.ds((n - 2) * (s.half), s.half)] = value.astype(bf16)

    def settle(self, j):
        for k in reversed(range(STAGES)):
            u = j - k

            @pl.when((u >= 0) & (u < self.s.units))
            def _(k=k, u=u):
                for m in ((0, 1), (2, 3)) if k == 0 else ():
                    for stream in self.streams:
                        stream.start(u, m)
                for n, stream in enumerate(self.streams if k else ()):
                    stream.stage(k, u, functools.partial(self.put, n))


def sums(s):
    return [array(s.units, 2, s.rows, PAIR), array(s.units, s.sub, s.d)]


def arrivals(s, sources, targets, sems):
    return [[pltpu.make_async_copy(src.at[part], dst.at[part], sems.at[n, m]) for m, (src, dst) in enumerate(zip(sources, targets, strict=True))] for n, part in enumerate(parts(s))]


def wait_first(j, arrive):
    @pl.when(j == 0)
    def _():
        for one in sum(arrive, []):
            one.wait()


def back_gates(both, by):
    gate, up, by = both[:, :UNIT], both[:, UNIT:], by.astype(f32)
    sig, act = silu_parts(gate)
    return (by * up * (sig + act * (1.0 - sig))).astype(bf16), (by * act).astype(bf16), (act * up).astype(bf16)


def second_kernel(s, acts_in, dys_in, wg, wd, g_early, d_early, dgux, g_late, theirs, out_g, out_d, acts, dys, gv, dv, dgu, prod, tiles_in, local, saved, given, sent, *refs):
    me = here()
    j = pl.program_id(0)
    streams = streams_of(me, s, gv.at[pl.ds(2, s.late)], dv.at[pl.ds(2, s.late)], refs[:8])
    terms = Terms(s, me, out_g, out_d, refs[8:])

    def at(k, u):
        at_stage(streams, k, u, s.late)

    def load(u):
        return [pltpu.make_async_copy(src.at[u], dst.at[flip(u)], local.at[n, flip(u)]) for n, (src, dst) in enumerate(((g_early, gv), (d_early, dv)))]

    arrive = arrivals(s, (acts_in, dys_in), (acts, dys), tiles_in)

    def place(u):
        return jnp.where(u < s.early, flip(u), u - s.early + 2)

    def save(u):
        return pltpu.make_async_copy(gv.at[place(u)], g_late.at[u - s.early], saved)

    def give(u):
        return remote(gv.at[place(u)], theirs.at[u], given.at[0, u], given.at[1, u], twin(me))

    def dgu_out(u):
        return split(s, me, dgu, dgux, u, PAIR, sent)

    @pl.when(j == 0)
    def _():
        y, z = me["y"], me["z"]
        rest = pl.ds(s.early, s.late)
        own = [pltpu.make_async_copy(src.at[1, rest], dst.at[pl.ds(2, s.late), y, z], local.at[2, n]) for n, (src, dst) in enumerate(((wg, gv), (wd, dv)))]
        for one in own + load(0) + load(1) + sum(arrive, []):
            one.start()
        greet(in_plane(me) + beside(me) + [twin(me)])
        for one in own:
            one.wait()
        early(streams, s.late, WARM[:1])

    for k in reversed(range(5)):
        at(k, j - k + 1)

    @pl.when((j >= 1) & (j <= s.units))
    def _():
        for one in (*dgu_out(j - 1), give(j - 1)):
            one.wait()

    @pl.when((j > s.early) & (j <= s.units))
    def _():
        save(j - 1).wait()

    @pl.when(j < s.units)
    def _():
        @pl.when(j < s.early)
        def _():
            for one in load(j):
                one.wait()

        @pl.when((j >= 1) & (j + 1 < s.early))
        def _():
            for one in load(j + 1):
                one.start()

        @pl.when(j >= s.early)
        def _():
            save(j).start()

        give(j).start()
        wait_first(j, arrive)
        now = place(j)
        weights, ahead = gv[now].reshape(s.d, PAIR), dv[now].reshape(UNIT, s.d)
        for part in parts(s):
            both = dot(acts[part], weights, NN)
            by = dot(dys[part], ahead, NT).astype(bf16)
            dgu[part, :UNIT], dgu[part, UNIT:], prod[part] = back_gates(both, by)
        terms.make(j, acts, dgu, prod, dys, dgu_out(j))

    terms.settle(j)


def second(s, acts, dys, wg, wd, g_early, d_early):
    unit, row = (*PLANE, s.pair, PAIR), (*PLANE, s.sub, s.d)
    return call(
        functools.partial(second_kernel, s),
        "second",
        3,
        grid=(s.units + STAGES - 1,),
        in_specs=[ANY] * 6,
        out_specs=[ANY] * 3 + [whole(one.shape) for one in sums(s)],
        out_shape=[array(s.tokens, 2 * s.wide), array(s.late, *unit), array(s.units, *unit), *sums(s)],
        scratch_shapes=[
            *[pltpu.VMEM((s.both, s.d), bf16)] * 2,
            pltpu.VMEM((2 + s.late, *unit), bf16),
            pltpu.VMEM((2 + s.late, *row), bf16),
            pltpu.VMEM((s.both, PAIR), bf16),
            pltpu.VMEM((s.both, UNIT), bf16),
            pltpu.SemaphoreType.DMA((4, 2)),
            pltpu.SemaphoreType.DMA((3, 2)),
            pltpu.SemaphoreType.DMA,
            pltpu.SemaphoreType.DMA((2, s.units)),
            pltpu.SemaphoreType.DMA((3, s.units)),
            *gather_sems(s.late),
            *terms_scratch(s),
        ],
    )(acts, dys, wg, wd, g_early, d_early)


def third_kernel(s, acts_in, dh_in, wd, gu, out_g, out_d, acts, dh, dgu, prod, tiles_in, *refs):
    me = here()
    j = pl.program_id(0)
    terms = Terms(s, me, out_g, out_d, refs)
    arrive = arrivals(s, (dh_in, acts_in), (dh, acts), tiles_in)

    @pl.when(j == 0)
    def _():
        for one in sum(arrive, []):
            one.start()
        greet(in_plane(me) + beside(me))

    @pl.when(j < s.units)
    def _():
        wait_first(j, arrive)
        ahead = wd[...]
        for part in parts(s):
            by = dot(dh[part], ahead, NT).astype(bf16)
            dgu[part, :UNIT], dgu[part, UNIT:], prod[part] = back_gates(gu[part], by)
        terms.make(j, acts, dgu, prod, dh)

    terms.settle(j)


def third(s, number, acts, dh, wd, gu):
    at = lambda j: jnp.minimum(j, s.units - 1)
    return call(
        functools.partial(third_kernel, s),
        "third",
        number,
        grid=(s.units + STAGES - 1,),
        in_specs=[ANY] * 2 + [pl.BlockSpec((UNIT, s.d), lambda j: (at(j), 0)), pl.BlockSpec((s.both, PAIR), lambda j: (0, at(j)))],
        out_specs=[whole(one.shape) for one in sums(s)],
        out_shape=sums(s),
        scratch_shapes=[
            *[pltpu.VMEM((s.both, s.d), bf16)] * 2,
            pltpu.VMEM((s.both, PAIR), bf16),
            pltpu.VMEM((s.both, UNIT), bf16),
            pltpu.SemaphoreType.DMA((4, 2)),
            *terms_scratch(s),
        ],
    )(acts, dh, wd, gu)


def adamw(w, m, v, g):
    m = 0.9 * m + 0.1 * g
    v = 0.95 * v + 0.05 * g * g
    step = m * lax.rsqrt(v + 1e-8) + 0.1 * w
    return (w - 0.02 * step).astype(bf16), m, v


def others(me):
    steps = [(y, z, c) for y in range(4) for z in range(4) for c in range(2)]
    return [{"y": ring(me["y"], y), "z": ring(me["z"], z), "c": flip(me["c"] + c)} for y, z, c in steps[1:]]


def total_kernel(g0, d0, g1, d1, got, out, sums, sent, here_got):
    me = here()
    greet(others(me))
    pairs = [remote(g.at[:, 1 - me["c"]], got.at[n], sent.at[n], here_got.at[n], twin(me)) for n, g in enumerate((g0, g1))]
    for one in pairs:
        one.start()
    total = sum(jnp.sum(g[...].astype(f32) ** 2) for g in (g0, d0, g1, d1))
    sums[0] = jnp.full(out.shape, total)
    for n, to in enumerate(others(me), 1):
        pairs.append(remote(sums.at[0], sums.at[n], sent.at[n + 1], here_got.at[n + 1], to))
        pairs[-1].start()
    for one in pairs:
        one.wait()
    out[...] = jnp.sum(sums[...], 0)


def total(number, *sums):
    tile, shape = (8, HALF), sums[0].shape
    sems = pltpu.SemaphoreType.DMA((33,))
    return call(
        total_kernel,
        "total",
        number,
        in_specs=[VMEM] * 4,
        out_specs=[VMEM] * 2,
        out_shape=[array(2, shape[0], *shape[2:]), array(*tile, dtype=f32)],
        scratch_shapes=[pltpu.VMEM((32, *tile), f32), sems, sems],
    )(*sums)


def finish_kernel(s, g0, d0, g1, d1, got, squares, *refs):
    old, new = refs[:9], refs[9:]
    c = lax.axis_index("c")
    count = 16 * (s.layers * s.pair * 32 * s.block * 3)
    factor = jnp.minimum(1.0, 0.5 * lax.rsqrt(squares[:1, :1] / count + 1e-30))
    moves = [(start, n, core * s.ff + to) for core in range(2) for to, n, start in places(s, core)]

    def update(n, at, g):
        w, m, v = (old[n + 3 * k] for k in range(3))
        made = adamw(w[at].astype(f32), m[at], v[at], g * factor)
        for k, value in enumerate(made):
            new[n + 3 * k][at] = value

    for layer, (g, d) in enumerate(((g0, d0), (g1, d1))):
        for mat in range(2):
            lanes = pl.ds(mat * UNIT, UNIT)
            pieces = [[ref[u, c, :, lanes] if ref is g else ref[layer, u, :, lanes] for u in range(s.units)] for ref in (g, got)]
            mine, other = (jnp.concatenate(piece, 1).astype(f32) for piece in pieces)
            both = jnp.concatenate([jnp.where(c == 0, mine, other), jnp.where(c == 0, other, mine)], 1)
            update(mat, layer, jnp.concatenate(tiles(both, 32 * s.block, moves), 1))
        update(2, (slice(None), layer), d[...].astype(f32).reshape(s.padded, s.d)[: s.block])


def finish(s, sums, got, squares, old):
    out = [array(*one.shape, dtype=one.dtype) for one in old]
    kernel = functools.partial(finish_kernel, s)
    return call(kernel, "finish", None, in_specs=[VMEM] * 15, out_specs=[VMEM] * 9, out_shape=out)(*sums, got, squares, *old)


def turned(arrays):
    return [one.swapaxes(0, 1) if n % 3 == 2 else one for n, one in enumerate(arrays)]


def solution(mesh):
    cut_mesh = Mesh(mesh.devices.reshape(mesh.shape["rep"], mesh.shape["r"], 4, 4, 2), ("rep", "x", "y", "z", "c"))

    def step(x, dy, *arrays):
        s = sizes(x.shape, arrays[0].shape, arrays[2].shape)
        arrays = turned(arrays)
        flat = (s.both, s.d)
        gates, downs = prepare(s, arrays[:3])
        gates = gates.reshape(s.layers, s.units, s.pair, PAIR)
        downs = downs.reshape(s.layers, s.units, s.sub, s.d)
        acts0, dys, gu0, prod0, wd0 = first(s, x[0], dy[0], gates, downs)
        h1, acts1, g_early, d_early = down(s, prod0, wd0.reshape(s.wide, s.d), x[0], gates, downs)
        dys, acts0, acts1 = (one.reshape(flat) for one in (dys, acts0, acts1))
        dgu1, g_late, theirs, *sums1 = second(s, acts1, dys, gates, downs, g_early, d_early)
        w = (one.reshape(-1, s.d, PAIR) for one in (g_early, g_late, theirs))
        dh = back(s, dgu1, *w, h1, dy[0]).reshape(flat)
        sums0 = third(s, 6, acts0, dh, wd0.reshape(-1, s.d), gu0)
        return tuple(turned(finish(s, (*sums0, *sums1), *total(7, *sums0, *sums1), arrays)))

    place = ("y", "z", "c")
    states, cut = P(("rep", "x", *place), None, None), P(None, place, None)
    return jax.shard_map(
        step,
        mesh=cut_mesh,
        in_specs=(states, states) + (cut,) * 9,
        out_specs=(P("rep", place, None),) * 9,
        check_vma=False,
    )
```

```python
import functools
import types

import jax
import jax.numpy as jnp
from jax import lax
from jax.experimental import pallas as pl
from jax.experimental.pallas import tpu as pltpu
from jax.sharding import Mesh
from jax.sharding import PartitionSpec as P

bf16, f32 = jnp.bfloat16, jnp.float32
BY_AXES = pl.DeviceIdType.MESH
NN, NT, TN = ((1,), (0,)), ((1,), (1,)), ((0,), (0,))
UNIT = 256
PAIR = 2 * UNIT
PLANE = 4, 4
CHIPS = 16
TILES = 8
ALL = pl.ds(0, 4)
HALVES = [pl.ds(n, 2) for n in (0, 2)]
EPS = 1e-6


def dot(a, b, how):
    return lax.dot_general(a, b, (how, ((), ())), preferred_element_type=f32)


def sizes(x_shape, gate_shape, down_shape):
    s = types.SimpleNamespace()
    s.layers, s.rows, _ = gate_shape
    s.tokens, s.d = x_shape[1:]
    s.block = down_shape[1]
    s.padded = -(-s.block // CHIPS) * CHIPS
    s.ff = CHIPS * s.padded
    s.units = s.ff // UNIT
    s.sub = UNIT // CHIPS
    s.early = s.units // 3
    s.late = s.units - s.early
    s.kept = 3
    s.summed = s.units - s.kept
    s.pair = 2 * s.rows
    s.both, s.wide, s.tile, s.half = 2 * s.tokens, 2 * s.ff, s.tokens // TILES, s.d // 2
    return s


def here():
    return {name: lax.axis_index(name) for name in ("x", "y", "z", "c")}


def ring(v, k):
    return lax.rem(v + k + 4, 4)


def flip(v):
    return lax.rem(v, 2)


def greet(partners, meanwhile=None):
    barrier = pltpu.get_barrier_semaphore()
    for one in partners:
        pl.semaphore_signal(barrier, inc=1, device_id=one, device_id_type=BY_AXES)
    if meanwhile:
        meanwhile()
    pl.semaphore_wait(barrier, len(partners))


def in_plane(me):
    return [{axis: ring(me[axis], k)} for axis in "yz" for k in (1, -1)]


def beside(me):
    n = lax.axis_size("x")
    return [{"x": lax.rem(me["x"] + k, n)} for k in (1, n - 1)]


def twin(me):
    return {"c": 1 - me["c"]}


def remote(src, dst, sent, got, to):
    return pltpu.make_async_remote_copy(src_ref=src, dst_ref=dst, send_sem=sent, recv_sem=got, device_id=to, device_id_type=BY_AXES)


class Gather:
    def __init__(self, me, slot, sent, got, a, b):
        self.me, self.slot, self.sent, self.got, self.a, self.b = me, slot, sent, got, a, b

    def copy(self, u, m):
        i, j, x = self.me[self.a], self.me[self.b], self.me["x"]
        turn = 1 - 2 * flip(u)
        way = 1 - 2 * flip(u + x)
        came = ring(j, -way)
        if m < 2:
            at, to = (i, j), {self.a: ring(i, 1 - 2 * m)}
        elif m == 2:
            at, to = (ring(i, -turn), j), {self.a: ring(i, turn)}
        elif m == 3:
            at, to = (ALL, j), {self.b: ring(j, way)}
        elif m == 4:
            at, to = (ALL, came), {self.b: ring(j, way)}
        else:
            at, to = (pl.ds(2 * m - 10, 2), came), beside(self.me)[m - 5]
        ref = self.slot(u, *(at if self.a == "y" else at[::-1]))
        return remote(ref, ref, self.sent.at[u, m], self.got.at[u, m], to)

    def stage(self, k, u):
        for m in ((), (0, 1), (2,), (3,), (4, 5, 6))[k]:
            self.copy(u, m).wait_recv()
        for m in ((0, 1), (2,), (3,), (4, 5, 6), ())[k]:
            self.copy(u, m).start()
        if k == 4:
            for m in range(7):
                self.copy(u, m).wait_send()


def gather_sems(units):
    return [pltpu.SemaphoreType.DMA((units, 7)) for _ in range(8)]


DEPTH = 4


STAGES = 7


class Scatter:
    def __init__(self, me, bufs, sent, got, a, b):
        self.me, self.sent, self.got, self.a, self.b = me, sent, got, a, b
        self.term, self.rm, self.sm, self.r0, self.r1, self.t, self.q, self.s0, self.s1, self.x0, self.x1, self.tb, self.z0, self.z1 = bufs

    @staticmethod
    def scratch(rows, cols, units):
        sizes = [(3, 4, 4), (3, 4), (DEPTH,)] + [(2, 4)] * 4 + [(2,)] * 7
        return [pltpu.VMEM((*size, rows, cols), bf16) for size in sizes] + [pltpu.SemaphoreType.DMA((units, 11))] * 2

    def group(self, u, i, part=ALL):
        at = (i, part) if self.a == "y" else (part, i)
        return self.term.at[(lax.rem(u, 3), *at)]

    def copy(self, u, m):
        i, j, x = self.me[self.a], self.me[self.b], self.me["x"]
        turn, two, far = 1 - 2 * flip(u), flip(u), lax.rem(u, DEPTH)
        sems = self.sent.at[u, m], self.got.at[u, m]
        if m < 6:
            h, way = m % 2, 1 - 2 * (m % 2)
            same, other = HALVES[h], HALVES[1 - h]
            src, dst = ((self.group(u, ring(i, 2), same), self.r0.at[two, same]), (self.group(u, ring(i, way), other), self.rm.at[lax.rem(u, 3), other]), (self.t.at[two, same], self.r1.at[two, same]))[m // 2]
            return remote(src, dst, *sems, {self.a: ring(i, way)})
        if m < 9:
            src, dst, way = ((self.q.at[two, ring(j, 2)], self.s0.at[two], turn), (self.q.at[two, ring(j, -turn)], self.sm.at[far], -turn), (self.tb.at[two], self.s1.at[two], turn))[m - 6]
            return remote(src, dst, *sems, {self.b: ring(j, way)})
        src, dst = ((self.z0, self.x0), (self.z1, self.x1))[m - 9]
        way = (1 - 2 * flip(x)) * (1 if (self.a == "y") == (m == 9) else -1)
        return remote(src.at[two], dst.at[two], *sems, {"x": ring(x, way)})

    def start(self, u, m):
        for one in m:
            self.copy(u, one).start()

    def stage(self, k, u, put=None):
        i, j = self.me[self.a], self.me[self.b]
        turn, two, far = 1 - 2 * flip(u), flip(u), lax.rem(u, DEPTH)
        near, spread, last = range(6), range(6, 9), range(9, 11)
        for m in ((), near[:2], near[2:], spread[:1], spread[1:], last[:1], last[1:])[k]:
            self.copy(u, m).wait_recv()
        for m in ((), (), near, (), spread, last[:1], last[1:])[k]:
            self.copy(u, m).wait_send()
        wide = lambda ref, *at: ref[at].astype(f32)
        if k == 1:
            for half, way in zip(HALVES, (1, -1), strict=True):
                self.t[two, half] = (self.group(u, ring(i, way), half)[...].astype(f32) + wide(self.r0, two, half)).astype(bf16)
        if k == 2:
            self.q[two] = (self.group(u, i)[...].astype(f32) + wide(self.r1, two) + wide(self.rm, lax.rem(u, 3))).astype(bf16)
        if k == 3:
            self.tb[two] = (wide(self.q, two, ring(j, turn)) + wide(self.s0, two)).astype(bf16)
        if k == 4:
            self.z0[two] = (wide(self.q, two, j) + wide(self.s1, two) + wide(self.sm, far)).astype(bf16)
        if k == 5:
            self.z1[two] = (wide(self.z0, two) + wide(self.x0, two)).astype(bf16)
        if k == 6:
            put(u, wide(self.z1, two) + wide(self.x1, two))
        self.start(u, ((), near[4:], spread[:2], spread[2:], last[:1], last[1:], ())[k])


def call(kernel, name, number, **kw):
    params = dict(vmem_limit_bytes=67043328)
    if number is not None:
        params |= dict(collective_id=number, has_side_effects=True)
    return pl.pallas_call(kernel, name=name, compiler_params=pltpu.CompilerParams(**params), **kw)


ANY = pl.BlockSpec(memory_space=pl.ANY)


def whole(shape):
    return pl.BlockSpec(shape, lambda *_: (0,) * len(shape), pipeline_mode=pl.Buffered(1))


AXES = ("y", "z"), ("z", "y")
HALF = UNIT // 2


def streams_of(me, s, gates, downs, sems):
    out = []
    for buf, width in ((gates, UNIT), (downs, s.half)):
        for n, axes in enumerate(AXES):
            slot = lambda u, y, z, buf=buf, lanes=pl.ds(n * width, width): buf.at[u, y, z, :, lanes]
            out.append(Gather(me, slot, *sems[2 * len(out) : 2 * len(out) + 2], *axes))
    return out


def early(streams, units, stages):
    for k, u in stages:
        at_stage(streams, k, jnp.int32(u), units)


def at_stage(streams, k, u, units):
    @pl.when((u >= 0) & (u < units))
    def _():
        for stream in streams:
            stream.stage(k, u)


def silu_parts(gate):
    s = jax.nn.sigmoid(gate)
    return s, gate * s


def tiles(value, width, moves):
    lane = lax.broadcasted_iota(jnp.int32, (value.shape[0], HALF), 1)
    out = [jnp.zeros((value.shape[0], HALF), value.dtype)] * (width // HALF)
    for to, n, start in moves:
        for k in range(to // HALF, (to + n - 1) // HALF + 1):
            base = k * HALF - to
            low, high = max(start + base, 0), min(start + base + HALF, value.shape[1])
            piece = value[:, low:high]
            if high - low < HALF:
                gap = jnp.zeros((value.shape[0], HALF - (high - low)), value.dtype)
                piece = jnp.concatenate([gap, piece] if low > start + base else [piece, gap], 1)
            out[k] = jnp.where((lane >= -base) & (lane < n - base), piece, out[k])
    return out


def places(s, core):
    for u in range(s.units):
        for q in range(CHIPS):
            n = min(s.sub, s.block - u * s.sub)
            if n > 0:
                yield u * UNIT + q * s.sub, n, (2 * q + core) * s.block + u * s.sub


def prepare_kernel(s, wg, wu, wd, gates, downs, halves, padded, sems):
    me = here()
    greet([twin(me)])
    for layer in range(s.layers):
        for mat, w in enumerate((wg, wu)):
            for core in range(2):
                for k, tile in enumerate(tiles(w[layer].astype(f32), s.ff, places(s, core))):
                    halves[core, layer, k // 2, :, pl.ds(mat * UNIT + k % 2 * HALF, HALF)] = tile.astype(bf16)
        padded[layer] = jnp.concatenate([wd[:, layer], jnp.zeros((s.padded - s.block, s.d), bf16)], 0)
    c = me["c"]
    give = remote(halves.at[1 - c], gates.at[:, :, c], sems.at[0], sems.at[1], twin(me))
    keep = pltpu.make_async_copy(halves.at[c], gates.at[:, :, c], sems.at[2])
    rest = pltpu.make_async_copy(padded, downs, sems.at[3])
    for one in (give, keep, rest):
        one.start()
    for one in (give, keep, rest):
        one.wait()


VMEM = pl.BlockSpec(memory_space=pltpu.VMEM)


def array(*shape, dtype=bf16):
    return jax.ShapeDtypeStruct(shape, dtype)


def prepare(s, weights):
    half, down = (s.layers, s.units, s.rows, PAIR), (s.layers, s.padded, s.d)
    return call(
        functools.partial(prepare_kernel, s),
        "prepare",
        8,
        in_specs=[VMEM] * 3,
        out_specs=[ANY] * 2,
        out_shape=[array(s.layers, s.units, 2, s.rows, PAIR), array(*down)],
        scratch_shapes=[pltpu.VMEM((2, *half), bf16), pltpu.VMEM(down, bf16), pltpu.SemaphoreType.DMA((4,))],
    )(*weights)


WARM = [(k, d - k) for d in range(4) for k in range(d + 1)]


def parts(s):
    tile = s.tokens // 2
    return [pl.ds(n * tile, tile) for n in range(4)]


def lanes_of(u, width=UNIT):
    return pl.ds(pl.multiple_of(u * width, width), width)


def split(s, me, src, dst, u, width, sems):
    keep = pltpu.make_async_copy(src.at[pl.ds(0, s.tokens)], dst.at[:, lanes_of(u, width)], sems.at[0, u])
    give = remote(src.at[pl.ds(s.tokens, s.tokens)], dst.at[:, lanes_of(s.units + u, width)], sems.at[1, u], sems.at[2, u], twin(me))
    return keep, give


def first_kernel(s, x, dy, w, wd, acts, dys, gu, prod, downs, xv, av, pv, buf, dbuf, local, pair, prods, shared, *sems):
    me = here()
    j = pl.program_id(0)
    streams = streams_of(me, s, buf, dbuf, sems)
    y, z = me["y"], me["z"]
    rows = s.tokens // 4
    own_part = [pl.ds(n * rows, rows) for n in range(4)]

    def act_out(h):
        return pltpu.make_async_copy(av.at[pl.ds(h * s.tokens, s.tokens)], acts.at[h], local.at[5 + h])

    def share(n):
        return remote(av.at[own_part[n]], av.at[pl.ds(s.tokens + n * rows, rows)], pair.at[0, n], pair.at[1, n], twin(me))

    def prod_out(u):
        return split(s, me, pv.at[flip(u)], prod, u, UNIT, prods)

    def down_out(u):
        give = remote(dbuf.at[u], downs.at[1, u], shared.at[0, u], shared.at[1, u], twin(me))
        return pltpu.make_async_copy(dbuf.at[u], downs.at[0, u], shared.at[2, u]), give

    keep = pltpu.make_async_copy(xv.at[1], dys.at[0], local.at[4])
    give = remote(xv.at[1], dys.at[1], pair.at[0, 4], pair.at[1, 4], twin(me))

    @pl.when(j == 0)
    def _():
        own = [pltpu.make_async_copy(src.at[0], dst.at[:, y, z], local.at[n]) for n, (src, dst) in enumerate(((w, buf), (wd, dbuf)))]
        own += [pltpu.make_async_copy(one, xv.at[n], local.at[2 + n]) for n, one in enumerate((x, dy))]
        for one in own:
            one.start()
        greet(in_plane(me) + beside(me) + [twin(me)])
        own[0].wait()
        own[1].wait()
        early(streams, s.units, WARM[:3])
        own[2].wait()
        for n in range(4):
            wide = xv[0, own_part[n]].astype(f32)
            scale = lax.rsqrt(jnp.mean(wide * wide, -1, keepdims=True) + EPS)
            av[own_part[n]] = (wide * scale).astype(bf16)
            share(n).start()
            early(streams, s.units, WARM[3 + n : 4 + n])
        act_out(0).start()
        own[3].wait()
        keep.start()
        give.start()
        early(streams, s.units, WARM[7:])
        for n in range(4):
            share(n).wait()
        act_out(1).start()

    for k in range(5):
        at_stage(streams, 4 - k, j + k, s.units)
    for one in down_out(j):
        one.start()

    @pl.when(j >= 2)
    def _():
        for one in prod_out(j - 2):
            one.wait()

    weights = buf[j].reshape(s.d, PAIR)
    for part in parts(s):
        both = dot(av[part], weights, NN)
        gu[part] = both
        pv[flip(j), part] = (silu_parts(both[:, :UNIT])[1] * both[:, UNIT:]).astype(bf16)
    for one in prod_out(j):
        one.start()

    @pl.when(j == s.units - 1)
    def _():
        for one in (keep, give, act_out(0), act_out(1), *prod_out(j - 1), *prod_out(j)):
            one.wait()
        for u in range(s.units):
            for one in down_out(u):
                one.wait()


def first(s, x, dy, w, wd):
    both = (2, s.tokens, s.d)
    return call(
        functools.partial(first_kernel, s),
        "first",
        0,
        grid=(s.units,),
        in_specs=[ANY] * 4,
        out_specs=[ANY, ANY, pl.BlockSpec((s.both, PAIR), lambda j: (0, j)), ANY, ANY],
        out_shape=[array(*both), array(*both), array(s.both, s.wide, dtype=f32), array(s.tokens, s.wide), array(2, s.units, *PLANE, s.sub, s.d)],
        scratch_shapes=[
            pltpu.VMEM(both, bf16),
            pltpu.VMEM((s.both, s.d), bf16),
            pltpu.VMEM((2, s.both, UNIT), bf16),
            pltpu.VMEM((s.units, *PLANE, s.pair, PAIR), bf16),
            pltpu.VMEM((s.units, *PLANE, s.sub, s.d), bf16),
            pltpu.SemaphoreType.DMA((7,)),
            pltpu.SemaphoreType.DMA((2, 5)),
            pltpu.SemaphoreType.DMA((3, s.units)),
            pltpu.SemaphoreType.DMA((3, s.units)),
            *gather_sems(s.units),
        ],
    )(x, dy, w, wd)


class Both:
    def __init__(self, s, me, out, total, made, sems):
        self.s, self.me, self.out, self.total, self.made, self.sems = s, me, out, total, made, sems

    @staticmethod
    def scratch(s):
        return [pltpu.VMEM((s.tile, s.d), f32), pltpu.VMEM((2, s.tile, s.d), bf16), pltpu.SemaphoreType.DMA((3, TILES))]

    def copies(self, t):
        part, src = pl.ds(pl.multiple_of(t * self.s.tile, self.s.tile), self.s.tile), self.made.at[flip(t)]
        keep = pltpu.make_async_copy(src, self.out.at[0, part], self.sems.at[0, t])
        return keep, remote(src, self.out.at[1, part], self.sems.at[1, t], self.sems.at[2, t], twin(self.me))

    def step(self, t, product, make):
        @pl.when(t > 2)
        def _():
            for one in self.copies(t - 3):
                one.wait()

        def finish():
            self.made[flip(t - 1)] = make(self.total[...])
            for one in self.copies(t - 1):
                one.start()

        @pl.when((t > 0) & (t < TILES))
        def _():
            finish()
            self.total[...] = product()

        @pl.when(t == TILES)
        def _():
            finish()
            for one in self.copies(t - 2) + self.copies(t - 1):
                one.wait()


def tile_spec(s, width, late):
    return pl.BlockSpec((s.tile, width), lambda t: (jnp.clip(t - late, 0, TILES - 1), 0))


def down_kernel(s, prod, w, h, wg, wd, h_out, acts, gates, downs, wv, gv, dv, local, saved, *refs):
    me = here()
    t = pl.program_id(0)
    both, streams = Both(s, me, acts, *refs[:3]), streams_of(me, s, gv, dv, refs[3:])
    thirds = [pl.ds(n * s.wide // 3, s.wide // 3) for n in range(3)]

    def out(u):
        return [pltpu.make_async_copy(src.at[u], dst.at[u], saved.at[n, u]) for n, (src, dst) in enumerate(((gv, gates), (dv, downs)))]

    def slot(n):
        for k in reversed(range(5)):
            at_stage(streams, k, n - 2 * k, s.early)

        @pl.when((n >= TILES) & (n < TILES + s.early))
        def _():
            for one in out(n - TILES):
                one.start()

    @pl.when(t == 0)
    def _():
        loads = [pltpu.make_async_copy(w.at[part], wv.at[part], local.at[n]) for n, part in enumerate(thirds)]
        own = [pltpu.make_async_copy(src.at[1, pl.ds(0, s.early)], dst.at[:, me["y"], me["z"]], local.at[3 + n]) for n, (src, dst) in enumerate(((wg, gv), (wd, dv)))]
        for one in own + loads:
            one.start()
        greet(in_plane(me) + beside(me) + [twin(me)])
        for one in own:
            one.wait()
        for n, part in enumerate(thirds):
            slot(jnp.int32(n))
            loads[n].wait()
            product = dot(prod[:, part], wv[part], NN)
            both.total[...] = both.total[...] + product if n else product

    @pl.when(t > 0)
    def _():
        slot(t + 2)

    def make(total):
        new = (h[...].astype(f32) + total.astype(bf16).astype(f32)).astype(bf16)
        h_out[...] = new
        wide = new.astype(f32)
        scale = lax.rsqrt(jnp.mean(wide * wide, -1, keepdims=True) + EPS)
        return (wide * scale).astype(bf16)

    both.step(t, lambda: dot(prod[...], wv[...], NN), make)

    @pl.when(t == TILES)
    def _():
        for u in range(s.early):
            for one in out(u):
                one.wait()


def down(s, prod, w, h, wg, wd):
    unit, row = (s.early, *PLANE, s.pair, PAIR), (s.early, *PLANE, s.sub, s.d)
    return call(
        functools.partial(down_kernel, s),
        "down",
        1,
        grid=(TILES + 1,),
        in_specs=[tile_spec(s, s.wide, 0), ANY, tile_spec(s, s.d, 1), ANY, ANY],
        out_specs=[tile_spec(s, s.d, 1), ANY, ANY, ANY],
        out_shape=[array(s.tokens, s.d), array(2, s.tokens, s.d), array(*unit), array(*row)],
        scratch_shapes=[
            pltpu.VMEM((s.wide, s.d), bf16),
            pltpu.VMEM(unit, bf16),
            pltpu.VMEM(row, bf16),
            pltpu.SemaphoreType.DMA((5,)),
            pltpu.SemaphoreType.DMA((2, s.early)),
            *Both.scratch(s),
            *gather_sems(s.early),
        ],
    )(prod, w, h, wg, wd)


def back_kernel(s, dgu, w0, w1, w2, h, by, kept_g, kept_d, out, out_g, out_d, wv, local, kept, *refs):
    me = here()
    t = pl.program_id(0)
    both, terms = Both(s, me, out, *refs[:3]), Terms(s, me, s.kept, out_g, out_d, refs[3:])
    units = [w.at[u] for w in (w0, w1, w2) for u in range(w.shape[0])]
    loads = [pltpu.make_async_copy(one, wv.at[:, pl.ds(n * PAIR, PAIR)], local.at[n]) for n, one in enumerate(units)]

    @pl.when(t == 0)
    def _():
        held = [pltpu.make_async_copy(src, term.at[v], sem) for v in range(s.kept) for term, src, sem in terms.kept(v, kept_g, kept_d, kept)]
        for load in held + loads:
            load.start()
        greet(in_plane(me) + beside(me) + [twin(me)])
        for load in held:
            load.wait()

    terms.settle(t)

    @pl.when(t == 0)
    def _():
        each = len(units) // 3
        for n in range(3):
            for load in loads[n * each : (n + 1) * each]:
                load.wait()
            part = pl.ds(n * each * PAIR, each * PAIR)
            product = dot(dgu[:, part], wv[:, part], NT)
            both.total[...] = both.total[...] + product if n else product

    def make(total):
        da = total.astype(bf16).astype(f32)
        wide = h[...].astype(f32)
        scale = lax.rsqrt(jnp.mean(wide * wide, -1, keepdims=True) + EPS)
        along = jnp.mean(da * wide, -1, keepdims=True)
        dh = (scale * da - wide * (scale * scale * scale * along)).astype(bf16)
        return (by[...].astype(f32) + dh.astype(f32)).astype(bf16)

    both.step(t, lambda: dot(dgu[...], wv[...], NT), make)


def back(s, dgu, w0, w1, w2, h, by, *kept):
    return call(
        functools.partial(back_kernel, s),
        "back",
        2,
        grid=(TILES + 1,),
        in_specs=[tile_spec(s, 2 * s.wide, 0), ANY, ANY, ANY, tile_spec(s, s.d, 1), tile_spec(s, s.d, 1), ANY, ANY],
        out_specs=[ANY] + [whole(one.shape) for one in sums(s, s.kept)],
        out_shape=[array(2, s.tokens, s.d), *sums(s, s.kept)],
        scratch_shapes=[
            pltpu.VMEM((s.d, 2 * s.wide), bf16),
            pltpu.SemaphoreType.DMA((2 * s.units,)),
            pltpu.SemaphoreType.DMA((s.kept, 4)),
            *Both.scratch(s),
            *terms_scratch(s, s.kept),
        ],
    )(dgu, w0, w1, w2, h, by, *kept)


def terms_scratch(s, units):
    return Scatter.scratch(s.pair, UNIT, units) * 2 + Scatter.scratch(s.sub, s.half, units) * 2


class Terms:
    def __init__(self, s, me, units, gates, downs, refs):
        self.s, self.units, self.gates, self.downs = s, units, gates, downs
        each = len(refs) // 4
        self.streams = [Scatter(me, refs[n * each : n * each + each - 2], *refs[n * each + each - 2 : n * each + each], *AXES[1 - n % 2]) for n in range(4)]

    def make(self, u, acts, dgu, prod, by, between=()):
        s, slot = self.s, lax.rem(u, 3)
        down = dot(prod[...], by[...], TN).astype(bf16)
        for n in range(2):
            self.streams[2 + n].term[slot] = down[:, n * s.half : (n + 1) * s.half].reshape(*PLANE, s.sub, s.half)
        for one in between:
            one.start()
        for k in range(2):
            both = dot(acts[:, k * s.half : (k + 1) * s.half], dgu[...], TN).astype(bf16)
            for n in range(2):
                self.streams[n].term[slot, HALVES[k]] = both[:, n * UNIT : (n + 1) * UNIT].reshape(2, 4, s.pair, UNIT)

    def put(self, n, u, value):
        s = self.s
        if n < 2:
            self.gates[u, :, :, pl.ds(n * UNIT, UNIT)] = value.reshape(2, s.rows, UNIT).astype(bf16)
        else:
            self.downs[u, :, pl.ds((n - 2) * (s.half), s.half)] = value.astype(bf16)

    def settle(self, j):
        for k in reversed(range(STAGES)):
            u = j - k

            @pl.when((u >= 0) & (u < self.units))
            def _(k=k, u=u):
                for m in ((0, 1), (2, 3)) if k == 0 else ():
                    for stream in self.streams:
                        stream.start(u, m)
                for n, stream in enumerate(self.streams if k else ()):
                    stream.stage(k, u, functools.partial(self.put, n))

    def kept(self, v, gates, downs, sems):
        return [(stream.term, (gates, downs)[n // 2].at[v, n % 2], sems.at[v, n]) for n, stream in enumerate(self.streams)]


def sums(s, units):
    return [array(units, 2, s.rows, PAIR), array(units, s.sub, s.d)]


def arrivals(s, sources, targets, sems):
    return [[pltpu.make_async_copy(src.at[part], dst.at[part], sems.at[n, m]) for m, (src, dst) in enumerate(zip(sources, targets, strict=True))] for n, part in enumerate(parts(s))]


def wait_first(j, arrive):
    @pl.when(j == 0)
    def _():
        for one in sum(arrive, []):
            one.wait()


def back_gates(both, by):
    gate, up, by = both[:, :UNIT], both[:, UNIT:], by.astype(f32)
    sig, act = silu_parts(gate)
    return (by * up * (sig + act * (1.0 - sig))).astype(bf16), (by * act).astype(bf16), (act * up).astype(bf16)


def second_kernel(s, acts_in, dys_in, wg, wd, g_early, d_early, dgux, g_late, theirs, kept_g, kept_d, out_g, out_d, acts, dys, gv, dv, dgu, prod, tiles_in, local, saved, given, sent, kept, *refs):
    me = here()
    j = pl.program_id(0)
    streams = streams_of(me, s, gv.at[pl.ds(2, s.late)], dv.at[pl.ds(2, s.late)], refs[:8])
    terms = Terms(s, me, s.summed, out_g, out_d, refs[8:])
    keeps = [[pltpu.make_async_copy(term.at[(s.summed + v) % 3], to, sem) for term, to, sem in terms.kept(v, kept_g, kept_d, kept)] for v in range(s.kept)]

    def at(k, u):
        at_stage(streams, k, u, s.late)

    def load(u):
        return [pltpu.make_async_copy(src.at[u], dst.at[flip(u)], local.at[n, flip(u)]) for n, (src, dst) in enumerate(((g_early, gv), (d_early, dv)))]

    arrive = arrivals(s, (acts_in, dys_in), (acts, dys), tiles_in)

    def place(u):
        return jnp.where(u < s.early, flip(u), u - s.early + 2)

    def save(u):
        return pltpu.make_async_copy(gv.at[place(u)], g_late.at[u - s.early], saved)

    def give(u):
        return remote(gv.at[place(u)], theirs.at[u], given.at[0, u], given.at[1, u], twin(me))

    def dgu_out(u):
        return split(s, me, dgu, dgux, u, PAIR, sent)

    @pl.when(j == 0)
    def _():
        y, z = me["y"], me["z"]
        rest = pl.ds(s.early, s.late)
        own = [pltpu.make_async_copy(src.at[1, rest], dst.at[pl.ds(2, s.late), y, z], local.at[2, n]) for n, (src, dst) in enumerate(((wg, gv), (wd, dv)))]
        for one in own + load(0) + load(1) + sum(arrive, []):
            one.start()
        greet(in_plane(me) + beside(me) + [twin(me)])
        for one in own:
            one.wait()
        early(streams, s.late, WARM[:1])

    for k in reversed(range(5)):
        at(k, j - k + 1)

    @pl.when((j >= 1) & (j <= s.units))
    def _():
        for one in (*dgu_out(j - 1), give(j - 1)):
            one.wait()

    @pl.when((j > s.early) & (j <= s.units))
    def _():
        save(j - 1).wait()

    @pl.when(j < s.units)
    def _():
        @pl.when(j < s.early)
        def _():
            for one in load(j):
                one.wait()

        @pl.when((j >= 1) & (j + 1 < s.early))
        def _():
            for one in load(j + 1):
                one.start()

        @pl.when(j >= s.early)
        def _():
            save(j).start()

        give(j).start()
        wait_first(j, arrive)
        now = place(j)
        weights, ahead = gv[now].reshape(s.d, PAIR), dv[now].reshape(UNIT, s.d)
        for part in parts(s):
            both = dot(acts[part], weights, NN)
            by = dot(dys[part], ahead, NT).astype(bf16)
            dgu[part, :UNIT], dgu[part, UNIT:], prod[part] = back_gates(both, by)
        terms.make(j, acts, dgu, prod, dys, dgu_out(j))

    for v, copies in enumerate(keeps):

        @pl.when(j == s.summed + v)
        def _(copies=copies):
            for one in copies:
                one.start()

    terms.settle(j)

    @pl.when(j == s.units)
    def _():
        for one in sum(keeps, []):
            one.wait()


def kept_shapes(s):
    return [array(s.kept, 2, *PLANE, s.pair, UNIT), array(s.kept, 2, *PLANE, s.sub, s.half)]


def second(s, acts, dys, wg, wd, g_early, d_early):
    unit, row = (*PLANE, s.pair, PAIR), (*PLANE, s.sub, s.d)
    return call(
        functools.partial(second_kernel, s),
        "second",
        3,
        grid=(s.summed + STAGES - 1,),
        in_specs=[ANY] * 6,
        out_specs=[ANY] * 5 + [whole(one.shape) for one in sums(s, s.summed)],
        out_shape=[array(s.tokens, 2 * s.wide), array(s.late, *unit), array(s.units, *unit), *kept_shapes(s), *sums(s, s.summed)],
        scratch_shapes=[
            *[pltpu.VMEM((s.both, s.d), bf16)] * 2,
            pltpu.VMEM((2 + s.late, *unit), bf16),
            pltpu.VMEM((2 + s.late, *row), bf16),
            pltpu.VMEM((s.both, PAIR), bf16),
            pltpu.VMEM((s.both, UNIT), bf16),
            pltpu.SemaphoreType.DMA((4, 2)),
            pltpu.SemaphoreType.DMA((3, 2)),
            pltpu.SemaphoreType.DMA,
            pltpu.SemaphoreType.DMA((2, s.units)),
            pltpu.SemaphoreType.DMA((3, s.units)),
            pltpu.SemaphoreType.DMA((s.kept, 4)),
            *gather_sems(s.late),
            *terms_scratch(s, s.summed),
        ],
    )(acts, dys, wg, wd, g_early, d_early)


def third_kernel(s, acts_in, dh_in, wd, gu, out_g, out_d, acts, dh, dgu, prod, tiles_in, *refs):
    me = here()
    j = pl.program_id(0)
    terms = Terms(s, me, s.units, out_g, out_d, refs)
    arrive = arrivals(s, (dh_in, acts_in), (dh, acts), tiles_in)

    @pl.when(j == 0)
    def _():
        for one in sum(arrive, []):
            one.start()
        greet(in_plane(me) + beside(me))

    @pl.when(j < s.units)
    def _():
        wait_first(j, arrive)
        ahead = wd[...]
        for part in parts(s):
            by = dot(dh[part], ahead, NT).astype(bf16)
            dgu[part, :UNIT], dgu[part, UNIT:], prod[part] = back_gates(gu[part], by)
        terms.make(j, acts, dgu, prod, dh)

    terms.settle(j)


def third(s, number, acts, dh, wd, gu):
    at = lambda j: jnp.minimum(j, s.units - 1)
    return call(
        functools.partial(third_kernel, s),
        "third",
        number,
        grid=(s.units + STAGES - 1,),
        in_specs=[ANY] * 2 + [pl.BlockSpec((UNIT, s.d), lambda j: (at(j), 0)), pl.BlockSpec((s.both, PAIR), lambda j: (0, at(j)))],
        out_specs=[whole(one.shape) for one in sums(s, s.units)],
        out_shape=sums(s, s.units),
        scratch_shapes=[
            *[pltpu.VMEM((s.both, s.d), bf16)] * 2,
            pltpu.VMEM((s.both, PAIR), bf16),
            pltpu.VMEM((s.both, UNIT), bf16),
            pltpu.SemaphoreType.DMA((4, 2)),
            *terms_scratch(s, s.units),
        ],
    )(acts, dh, wd, gu)


def adamw(w, m, v, g):
    m = 0.9 * m + 0.1 * g
    v = 0.95 * v + 0.05 * g * g
    step = m * lax.rsqrt(v + 1e-8) + 0.1 * w
    return (w - 0.02 * step).astype(bf16), m, v


def others(me):
    steps = [(y, z, c) for y in range(4) for z in range(4) for c in range(2)]
    return [{"y": ring(me["y"], y), "z": ring(me["z"], z), "c": flip(me["c"] + c)} for y, z, c in steps[1:]]


def total_kernel(s, g0, d0, g1, d1, g2, d2, out, squares, sums, got0, got1, got2, sent, here_got):
    me = here()
    c = me["c"]

    def add_up():
        total = sum(jnp.sum(g[...].astype(f32) ** 2) for g in (g0, d0, g1, d1, g2, d2))
        sums[0] = jnp.full(squares.shape, total)

    greet(others(me), add_up)
    exchanged = (g0, got0), (g1, got1), (g2, got2)
    pairs = [remote(g.at[:, 1 - c], got, sent.at[n], here_got.at[n], twin(me)) for n, (g, got) in enumerate(exchanged)]
    for one in pairs:
        one.start()
    copies = [remote(sums.at[0], sums.at[n], sent.at[n + 2], here_got.at[n + 2], to) for n, to in enumerate(others(me), 1)]
    for one in copies:
        one.start()
    for one in pairs:
        one.wait()
    moves = [(start, n, core * s.ff + to) for core in range(2) for to, n, start in places(s, core)]
    for layer, refs in enumerate((exchanged[:1], exchanged[1:])):
        for mat in range(2):
            lanes = pl.ds(mat * UNIT, UNIT)
            mine = jnp.concatenate([g[u, c, :, lanes] for g, _ in refs for u in range(g.shape[0])], 1).astype(f32)
            other = jnp.concatenate([got[u, :, lanes] for _, got in refs for u in range(got.shape[0])], 1).astype(f32)
            both = jnp.concatenate([jnp.where(c == 0, mine, other), jnp.where(c == 0, other, mine)], 1)
            out[layer, mat] = jnp.concatenate(tiles(both, 32 * s.block, moves), 1).astype(bf16)
    for one in copies:
        one.wait()
    squares[...] = jnp.sum(sums[...], 0)


def total(s, number, *sums):
    tile = (8, HALF)
    sems = pltpu.SemaphoreType.DMA((34,))
    return call(
        functools.partial(total_kernel, s),
        "total",
        number,
        in_specs=[VMEM] * 6,
        out_specs=[VMEM] * 2,
        out_shape=[array(s.layers, 2, s.rows, 32 * s.block), array(*tile, dtype=f32)],
        scratch_shapes=[pltpu.VMEM((32, *tile), f32), *[pltpu.VMEM((g.shape[0], *g.shape[2:]), bf16) for g in sums[::2]], sems, sems],
    )(*sums)


def finish_kernel(s, g, d0, d1, d2, squares, *refs):
    old, new, bufs, (ins, outs) = refs[:9], refs[9:18], refs[18:27], refs[27:]
    loads = [pltpu.make_async_copy(src, dst, ins.at[n]) for n, (src, dst) in enumerate(zip(old, bufs, strict=True))]
    stores = [pltpu.make_async_copy(src, dst, outs.at[n]) for n, (src, dst) in enumerate(zip(bufs, new, strict=True))]
    for n in range(3):
        for load in loads[n::3]:
            load.start()
    count = s.layers * s.d * 32 * s.block * 3
    factor = jnp.minimum(1.0, 0.5 * lax.rsqrt(squares[:1, :1] / count + 1e-30))
    for n in range(3):
        for load in loads[n::3]:
            load.wait()
        for layer in range(s.layers):
            if n < 2:
                at, grad = layer, g[layer, n].astype(f32)
            else:
                rows = jnp.concatenate([one[...] for one in ((d1, d2) if layer else (d0,))], 0).reshape(s.padded, s.d)
                at, grad = (slice(None), layer), rows[: s.block].astype(f32)
            w, m, v = bufs[n::3]
            made = adamw(w[at].astype(f32), m[at], v[at], grad * factor)
            for ref, value in zip((w, m, v), made, strict=True):
                ref[at] = value
        for store in stores[n::3]:
            store.start()
    for store in stores:
        store.wait()


def finish(s, g, downs, squares, old):
    out = [array(*one.shape, dtype=one.dtype) for one in old]
    sems = pltpu.SemaphoreType.DMA((9,))
    kernel = functools.partial(finish_kernel, s)
    scratch = [pltpu.VMEM(one.shape, one.dtype) for one in old] + [sems, sems]
    return call(kernel, "finish", None, in_specs=[VMEM] * 5 + [ANY] * 9, out_specs=[ANY] * 9, out_shape=out, scratch_shapes=scratch)(g, *downs, squares, *old)


def turned(arrays):
    return [one.swapaxes(0, 1) if n % 3 == 2 else one for n, one in enumerate(arrays)]


def solution(mesh):
    cut_mesh = Mesh(mesh.devices.reshape(mesh.shape["rep"], mesh.shape["r"], 4, 4, 2), ("rep", "x", "y", "z", "c"))

    def step(x, dy, *arrays):
        s = sizes(x.shape, arrays[0].shape, arrays[2].shape)
        arrays = turned(arrays)
        flat = (s.both, s.d)
        gates, downs = prepare(s, arrays[:3])
        gates = gates.reshape(s.layers, s.units, s.pair, PAIR)
        downs = downs.reshape(s.layers, s.units, s.sub, s.d)
        acts0, dys, gu0, prod0, wd0 = first(s, x[0], dy[0], gates, downs)
        h1, acts1, g_early, d_early = down(s, prod0, wd0.reshape(s.wide, s.d), x[0], gates, downs)
        dys, acts0, acts1 = (one.reshape(flat) for one in (dys, acts0, acts1))
        dgu1, g_late, theirs, kept_g, kept_d, *sums1 = second(s, acts1, dys, gates, downs, g_early, d_early)
        w = (one.reshape(-1, s.d, PAIR) for one in (g_early, g_late, theirs))
        dh, *sums2 = back(s, dgu1, *w, h1, dy[0], kept_g, kept_d)
        dh = dh.reshape(flat)
        sums0 = third(s, 6, acts0, dh, wd0.reshape(-1, s.d), gu0)
        every = (*sums0, *sums1, *sums2)
        g, squares = total(s, 7, *every)
        return tuple(turned(finish(s, g, every[1::2], squares, arrays)))

    place = ("y", "z", "c")
    states, cut = P(("rep", "x", *place), None, None), P(None, place, None)
    return jax.shard_map(
        step,
        mesh=cut_mesh,
        in_specs=(states, states) + (cut,) * 9,
        out_specs=(P("rep", place, None),) * 9,
        check_vma=False,
    )
```

```python
import functools
import types

import jax
import jax.numpy as jnp
from jax import lax
from jax.experimental import pallas as pl
from jax.experimental.pallas import tpu as pltpu
from jax.sharding import Mesh
from jax.sharding import PartitionSpec as P

bf16, f32 = jnp.bfloat16, jnp.float32
BY_AXES = pl.DeviceIdType.MESH
NN, NT, TN = ((1,), (0,)), ((1,), (1,)), ((0,), (0,))
UNIT = 256
PAIR = 2 * UNIT
PLANE = 4, 4
CHIPS = 16
TILES = 8
ALL = pl.ds(0, 4)
HALVES = [pl.ds(n, 2) for n in (0, 2)]
EPS = 1e-6


def dot(a, b, how):
    return lax.dot_general(a, b, (how, ((), ())), preferred_element_type=f32)


def sizes(x_shape, gate_shape, down_shape):
    s = types.SimpleNamespace()
    s.layers, s.rows, _ = gate_shape
    s.tokens, s.d = x_shape[1:]
    s.block = down_shape[1]
    s.padded = -(-s.block // CHIPS) * CHIPS
    s.ff = CHIPS * s.padded
    s.units = s.ff // UNIT
    s.sub = UNIT // CHIPS
    s.early = s.units // 3
    s.late = s.units - s.early
    s.kept = 3
    s.summed = s.units - s.kept
    s.pair = 2 * s.rows
    s.both, s.wide, s.tile, s.half = 2 * s.tokens, 2 * s.ff, s.tokens // TILES, s.d // 2
    return s


def here():
    return {name: lax.axis_index(name) for name in ("x", "y", "z", "c")}


def ring(v, k):
    return lax.rem(v + k + 4, 4)


def flip(v):
    return lax.rem(v, 2)


def greet(partners, meanwhile=None):
    barrier = pltpu.get_barrier_semaphore()
    for one in partners:
        pl.semaphore_signal(barrier, inc=1, device_id=one, device_id_type=BY_AXES)
    if meanwhile:
        meanwhile()
    pl.semaphore_wait(barrier, len(partners))


def in_plane(me):
    return [{axis: ring(me[axis], k)} for axis in "yz" for k in (1, -1)]


def beside(me):
    n = lax.axis_size("x")
    return [{"x": lax.rem(me["x"] + k, n)} for k in (1, n - 1)]


def twin(me):
    return {"c": 1 - me["c"]}


def remote(src, dst, sent, got, to):
    return pltpu.make_async_remote_copy(src_ref=src, dst_ref=dst, send_sem=sent, recv_sem=got, device_id=to, device_id_type=BY_AXES)


class Gather:
    def __init__(self, me, slot, sent, got, a, b):
        self.me, self.slot, self.sent, self.got, self.a, self.b = me, slot, sent, got, a, b

    def copy(self, u, m):
        i, j, x = self.me[self.a], self.me[self.b], self.me["x"]
        turn = 1 - 2 * flip(u)
        way = 1 - 2 * flip(u + x)
        came = ring(j, -way)
        if m < 2:
            at, to = (i, j), {self.a: ring(i, 1 - 2 * m)}
        elif m == 2:
            at, to = (ring(i, -turn), j), {self.a: ring(i, turn)}
        elif m == 3:
            at, to = (ALL, j), {self.b: ring(j, way)}
        elif m == 4:
            at, to = (ALL, came), {self.b: ring(j, way)}
        else:
            at, to = (pl.ds(2 * m - 10, 2), came), beside(self.me)[m - 5]
        ref = self.slot(u, *(at if self.a == "y" else at[::-1]))
        return remote(ref, ref, self.sent.at[u, m], self.got.at[u, m], to)

    def stage(self, k, u):
        for m in ((), (0, 1), (2,), (3,), (4, 5, 6))[k]:
            self.copy(u, m).wait_recv()
        for m in ((0, 1), (2,), (3,), (4, 5, 6), ())[k]:
            self.copy(u, m).start()
        if k == 4:
            for m in range(7):
                self.copy(u, m).wait_send()


def gather_sems(units):
    return [pltpu.SemaphoreType.DMA((units, 7)) for _ in range(8)]


DEPTH = 4


STAGES = 7


class Scatter:
    def __init__(self, me, bufs, sent, got, a, b):
        self.me, self.sent, self.got, self.a, self.b = me, sent, got, a, b
        self.term, self.rm, self.sm, self.r0, self.r1, self.t, self.q, self.s0, self.s1, self.x0, self.x1, self.tb, self.z0, self.z1 = bufs

    @staticmethod
    def scratch(rows, cols, units):
        sizes = [(3, 4, 4), (3, 4), (DEPTH,)] + [(2, 4)] * 4 + [(2,)] * 7
        return [pltpu.VMEM((*size, rows, cols), bf16) for size in sizes] + [pltpu.SemaphoreType.DMA((units, 11))] * 2

    def group(self, u, i, part=ALL):
        at = (i, part) if self.a == "y" else (part, i)
        return self.term.at[(lax.rem(u, 3), *at)]

    def copy(self, u, m):
        i, j, x = self.me[self.a], self.me[self.b], self.me["x"]
        turn, two, far = 1 - 2 * flip(u), flip(u), lax.rem(u, DEPTH)
        sems = self.sent.at[u, m], self.got.at[u, m]
        if m < 6:
            h, way = m % 2, 1 - 2 * (m % 2)
            same, other = HALVES[h], HALVES[1 - h]
            src, dst = ((self.group(u, ring(i, 2), same), self.r0.at[two, same]), (self.group(u, ring(i, way), other), self.rm.at[lax.rem(u, 3), other]), (self.t.at[two, same], self.r1.at[two, same]))[m // 2]
            return remote(src, dst, *sems, {self.a: ring(i, way)})
        if m < 9:
            src, dst, way = ((self.q.at[two, ring(j, 2)], self.s0.at[two], turn), (self.q.at[two, ring(j, -turn)], self.sm.at[far], -turn), (self.tb.at[two], self.s1.at[two], turn))[m - 6]
            return remote(src, dst, *sems, {self.b: ring(j, way)})
        src, dst = ((self.z0, self.x0), (self.z1, self.x1))[m - 9]
        way = (1 - 2 * flip(x)) * (1 if (self.a == "y") == (m == 9) else -1)
        return remote(src.at[two], dst.at[two], *sems, {"x": ring(x, way)})

    def start(self, u, m):
        for one in m:
            self.copy(u, one).start()

    def stage(self, k, u, put=None):
        i, j = self.me[self.a], self.me[self.b]
        turn, two, far = 1 - 2 * flip(u), flip(u), lax.rem(u, DEPTH)
        near, spread, last = range(6), range(6, 9), range(9, 11)
        for m in ((), near[:2], near[2:], spread[:1], spread[1:], last[:1], last[1:])[k]:
            self.copy(u, m).wait_recv()
        for m in ((), (), near, (), spread, last[:1], last[1:])[k]:
            self.copy(u, m).wait_send()
        wide = lambda ref, *at: ref[at].astype(f32)
        if k == 1:
            for half, way in zip(HALVES, (1, -1), strict=True):
                self.t[two, half] = (self.group(u, ring(i, way), half)[...].astype(f32) + wide(self.r0, two, half)).astype(bf16)
        if k == 2:
            self.q[two] = (self.group(u, i)[...].astype(f32) + wide(self.r1, two) + wide(self.rm, lax.rem(u, 3))).astype(bf16)
        if k == 3:
            self.tb[two] = (wide(self.q, two, ring(j, turn)) + wide(self.s0, two)).astype(bf16)
        if k == 4:
            self.z0[two] = (wide(self.q, two, j) + wide(self.s1, two) + wide(self.sm, far)).astype(bf16)
        if k == 5:
            self.z1[two] = (wide(self.z0, two) + wide(self.x0, two)).astype(bf16)
        if k == 6:
            put(u, wide(self.z1, two) + wide(self.x1, two))
        self.start(u, ((), near[4:], spread[:2], spread[2:], last[:1], last[1:], ())[k])


def call(kernel, name, number, **kw):
    params = dict(vmem_limit_bytes=67043328)
    if number is not None:
        params |= dict(collective_id=number, has_side_effects=True)
    return pl.pallas_call(kernel, name=name, compiler_params=pltpu.CompilerParams(**params), **kw)


ANY = pl.BlockSpec(memory_space=pl.ANY)


def whole(shape):
    return pl.BlockSpec(shape, lambda *_: (0,) * len(shape), pipeline_mode=pl.Buffered(1))


AXES = ("y", "z"), ("z", "y")
HALF = UNIT // 2


def streams_of(me, s, gates, downs, sems):
    out = []
    for buf, width in ((gates, UNIT), (downs, s.half)):
        for n, axes in enumerate(AXES):
            slot = lambda u, y, z, buf=buf, lanes=pl.ds(n * width, width): buf.at[u, y, z, :, lanes]
            out.append(Gather(me, slot, *sems[2 * len(out) : 2 * len(out) + 2], *axes))
    return out


def early(streams, units, stages):
    for k, u in stages:
        at_stage(streams, k, jnp.int32(u), units)


def at_stage(streams, k, u, units):
    @pl.when((u >= 0) & (u < units))
    def _():
        for stream in streams:
            stream.stage(k, u)


def silu_parts(gate):
    s = jax.nn.sigmoid(gate)
    return s, gate * s


def tiles(value, width, moves):
    lane = lax.broadcasted_iota(jnp.int32, (value.shape[0], HALF), 1)
    out = [jnp.zeros((value.shape[0], HALF), value.dtype)] * (width // HALF)
    for to, n, start in moves:
        for k in range(to // HALF, (to + n - 1) // HALF + 1):
            base = k * HALF - to
            low, high = max(start + base, 0), min(start + base + HALF, value.shape[1])
            piece = value[:, low:high]
            if high - low < HALF:
                gap = jnp.zeros((value.shape[0], HALF - (high - low)), value.dtype)
                piece = jnp.concatenate([gap, piece] if low > start + base else [piece, gap], 1)
            out[k] = jnp.where((lane >= -base) & (lane < n - base), piece, out[k])
    return out


def places(s, core):
    for u in range(s.units):
        for q in range(CHIPS):
            n = min(s.sub, s.block - u * s.sub)
            if n > 0:
                yield u * UNIT + q * s.sub, n, (2 * q + core) * s.block + u * s.sub


def prepare_kernel(s, wg, wu, wd, gates, downs, halves, padded, sems):
    me = here()

    def arrange():
        for layer in range(s.layers):
            for mat, w in enumerate((wg, wu)):
                for core in range(2):
                    for k, tile in enumerate(tiles(w[layer].astype(f32), s.ff, places(s, core))):
                        halves[core, layer, k // 2, :, pl.ds(mat * UNIT + k % 2 * HALF, HALF)] = tile.astype(bf16)
            padded[layer] = jnp.concatenate([wd[:, layer], jnp.zeros((s.padded - s.block, s.d), bf16)], 0)

    greet([twin(me)], arrange)
    c = me["c"]
    give = remote(halves.at[1 - c], gates.at[:, :, c], sems.at[0], sems.at[1], twin(me))
    keep = pltpu.make_async_copy(halves.at[c], gates.at[:, :, c], sems.at[2])
    rest = pltpu.make_async_copy(padded, downs, sems.at[3])
    for one in (give, keep, rest):
        one.start()
    for one in (give, keep, rest):
        one.wait()


VMEM = pl.BlockSpec(memory_space=pltpu.VMEM)


def array(*shape, dtype=bf16):
    return jax.ShapeDtypeStruct(shape, dtype)


def prepare(s, weights):
    half, down = (s.layers, s.units, s.rows, PAIR), (s.layers, s.padded, s.d)
    return call(
        functools.partial(prepare_kernel, s),
        "prepare",
        8,
        in_specs=[VMEM] * 3,
        out_specs=[ANY] * 2,
        out_shape=[array(s.layers, s.units, 2, s.rows, PAIR), array(*down)],
        scratch_shapes=[pltpu.VMEM((2, *half), bf16), pltpu.VMEM(down, bf16), pltpu.SemaphoreType.DMA((4,))],
    )(*weights)


WARM = [(k, d - k) for d in range(4) for k in range(d + 1)]


def parts(s):
    tile = s.tokens // 2
    return [pl.ds(n * tile, tile) for n in range(4)]


def lanes_of(u, width=UNIT):
    return pl.ds(pl.multiple_of(u * width, width), width)


def split(s, me, src, dst, u, width, sems):
    keep = pltpu.make_async_copy(src.at[pl.ds(0, s.tokens)], dst.at[:, lanes_of(u, width)], sems.at[0, u])
    give = remote(src.at[pl.ds(s.tokens, s.tokens)], dst.at[:, lanes_of(s.units + u, width)], sems.at[1, u], sems.at[2, u], twin(me))
    return keep, give


def first_kernel(s, x, dy, w, wd, acts, dys, gu, prod, downs, xv, av, pv, buf, dbuf, local, pair, prods, shared, *sems):
    me = here()
    j = pl.program_id(0)
    streams = streams_of(me, s, buf, dbuf, sems)
    y, z = me["y"], me["z"]
    rows = s.tokens // 4
    own_part = [pl.ds(n * rows, rows) for n in range(4)]

    def act_out(h):
        return pltpu.make_async_copy(av.at[pl.ds(h * s.tokens, s.tokens)], acts.at[h], local.at[5 + h])

    def share(n):
        return remote(av.at[own_part[n]], av.at[pl.ds(s.tokens + n * rows, rows)], pair.at[0, n], pair.at[1, n], twin(me))

    def prod_out(u):
        return split(s, me, pv.at[flip(u)], prod, u, UNIT, prods)

    def down_out(u):
        give = remote(dbuf.at[u], downs.at[1, u], shared.at[0, u], shared.at[1, u], twin(me))
        return pltpu.make_async_copy(dbuf.at[u], downs.at[0, u], shared.at[2, u]), give

    keep = pltpu.make_async_copy(xv.at[1], dys.at[0], local.at[4])
    give = remote(xv.at[1], dys.at[1], pair.at[0, 4], pair.at[1, 4], twin(me))

    @pl.when(j == 0)
    def _():
        own = [pltpu.make_async_copy(src.at[0], dst.at[:, y, z], local.at[n]) for n, (src, dst) in enumerate(((w, buf), (wd, dbuf)))]
        own += [pltpu.make_async_copy(one, xv.at[n], local.at[2 + n]) for n, one in enumerate((x, dy))]
        for one in own:
            one.start()
        greet(in_plane(me) + beside(me) + [twin(me)])
        own[0].wait()
        own[1].wait()
        early(streams, s.units, WARM[:3])
        own[2].wait()
        for n in range(4):
            wide = xv[0, own_part[n]].astype(f32)
            scale = lax.rsqrt(jnp.mean(wide * wide, -1, keepdims=True) + EPS)
            av[own_part[n]] = (wide * scale).astype(bf16)
            share(n).start()
            early(streams, s.units, WARM[3 + n : 4 + n])
        act_out(0).start()
        own[3].wait()
        keep.start()
        give.start()
        early(streams, s.units, WARM[7:])
        for n in range(4):
            share(n).wait()
        act_out(1).start()

    for k in range(5):
        at_stage(streams, 4 - k, j + k, s.units)
    for one in down_out(j):
        one.start()

    @pl.when(j >= 2)
    def _():
        for one in prod_out(j - 2):
            one.wait()

    weights = buf[j].reshape(s.d, PAIR)
    for part in parts(s):
        both = dot(av[part], weights, NN)
        gu[part] = both
        pv[flip(j), part] = (silu_parts(both[:, :UNIT])[1] * both[:, UNIT:]).astype(bf16)
    for one in prod_out(j):
        one.start()

    @pl.when(j == s.units - 1)
    def _():
        for one in (keep, give, act_out(0), act_out(1), *prod_out(j - 1), *prod_out(j)):
            one.wait()
        for u in range(s.units):
            for one in down_out(u):
                one.wait()


def first(s, x, dy, w, wd):
    both = (2, s.tokens, s.d)
    return call(
        functools.partial(first_kernel, s),
        "first",
        0,
        grid=(s.units,),
        in_specs=[ANY] * 4,
        out_specs=[ANY, ANY, pl.BlockSpec((s.both, PAIR), lambda j: (0, j)), ANY, ANY],
        out_shape=[array(*both), array(*both), array(s.both, s.wide, dtype=f32), array(s.tokens, s.wide), array(2, s.units, *PLANE, s.sub, s.d)],
        scratch_shapes=[
            pltpu.VMEM(both, bf16),
            pltpu.VMEM((s.both, s.d), bf16),
            pltpu.VMEM((2, s.both, UNIT), bf16),
            pltpu.VMEM((s.units, *PLANE, s.pair, PAIR), bf16),
            pltpu.VMEM((s.units, *PLANE, s.sub, s.d), bf16),
            pltpu.SemaphoreType.DMA((7,)),
            pltpu.SemaphoreType.DMA((2, 5)),
            pltpu.SemaphoreType.DMA((3, s.units)),
            pltpu.SemaphoreType.DMA((3, s.units)),
            *gather_sems(s.units),
        ],
    )(x, dy, w, wd)


class Both:
    def __init__(self, s, me, out, total, made, sems):
        self.s, self.me, self.out, self.total, self.made, self.sems = s, me, out, total, made, sems

    @staticmethod
    def scratch(s):
        return [pltpu.VMEM((s.tile, s.d), f32), pltpu.VMEM((2, s.tile, s.d), bf16), pltpu.SemaphoreType.DMA((3, TILES))]

    def copies(self, t):
        part, src = pl.ds(pl.multiple_of(t * self.s.tile, self.s.tile), self.s.tile), self.made.at[flip(t)]
        keep = pltpu.make_async_copy(src, self.out.at[0, part], self.sems.at[0, t])
        return keep, remote(src, self.out.at[1, part], self.sems.at[1, t], self.sems.at[2, t], twin(self.me))

    def step(self, t, product, make):
        @pl.when(t > 2)
        def _():
            for one in self.copies(t - 3):
                one.wait()

        def finish():
            self.made[flip(t - 1)] = make(self.total[...])
            for one in self.copies(t - 1):
                one.start()

        @pl.when((t > 0) & (t < TILES))
        def _():
            finish()
            self.total[...] = product()

        @pl.when(t == TILES)
        def _():
            finish()
            for one in self.copies(t - 2) + self.copies(t - 1):
                one.wait()


def tile_spec(s, width, late):
    return pl.BlockSpec((s.tile, width), lambda t: (jnp.clip(t - late, 0, TILES - 1), 0))


def down_kernel(s, prod, w, h, wg, wd, h_out, acts, gates, downs, wv, gv, dv, local, saved, *refs):
    me = here()
    t = pl.program_id(0)
    both, streams = Both(s, me, acts, *refs[:3]), streams_of(me, s, gv, dv, refs[3:])
    thirds = [pl.ds(n * s.wide // 3, s.wide // 3) for n in range(3)]

    def out(u):
        return [pltpu.make_async_copy(src.at[u], dst.at[u], saved.at[n, u]) for n, (src, dst) in enumerate(((gv, gates), (dv, downs)))]

    def slot(n):
        for k in reversed(range(5)):
            at_stage(streams, k, n - 2 * k, s.early)

        @pl.when((n >= TILES) & (n < TILES + s.early))
        def _():
            for one in out(n - TILES):
                one.start()

    @pl.when(t == 0)
    def _():
        loads = [pltpu.make_async_copy(w.at[part], wv.at[part], local.at[n]) for n, part in enumerate(thirds)]
        own = [pltpu.make_async_copy(src.at[1, pl.ds(0, s.early)], dst.at[:, me["y"], me["z"]], local.at[3 + n]) for n, (src, dst) in enumerate(((wg, gv), (wd, dv)))]
        for one in own + loads:
            one.start()
        greet(in_plane(me) + beside(me) + [twin(me)])
        for one in own:
            one.wait()
        for n, part in enumerate(thirds):
            slot(jnp.int32(n))
            loads[n].wait()
            product = dot(prod[:, part], wv[part], NN)
            both.total[...] = both.total[...] + product if n else product

    @pl.when(t > 0)
    def _():
        slot(t + 2)

    def make(total):
        new = (h[...].astype(f32) + total.astype(bf16).astype(f32)).astype(bf16)
        h_out[...] = new
        wide = new.astype(f32)
        scale = lax.rsqrt(jnp.mean(wide * wide, -1, keepdims=True) + EPS)
        return (wide * scale).astype(bf16)

    both.step(t, lambda: dot(prod[...], wv[...], NN), make)

    @pl.when(t == TILES)
    def _():
        for u in range(s.early):
            for one in out(u):
                one.wait()


def down(s, prod, w, h, wg, wd):
    unit, row = (s.early, *PLANE, s.pair, PAIR), (s.early, *PLANE, s.sub, s.d)
    return call(
        functools.partial(down_kernel, s),
        "down",
        1,
        grid=(TILES + 1,),
        in_specs=[tile_spec(s, s.wide, 0), ANY, tile_spec(s, s.d, 1), ANY, ANY],
        out_specs=[tile_spec(s, s.d, 1), ANY, ANY, ANY],
        out_shape=[array(s.tokens, s.d), array(2, s.tokens, s.d), array(*unit), array(*row)],
        scratch_shapes=[
            pltpu.VMEM((s.wide, s.d), bf16),
            pltpu.VMEM(unit, bf16),
            pltpu.VMEM(row, bf16),
            pltpu.SemaphoreType.DMA((5,)),
            pltpu.SemaphoreType.DMA((2, s.early)),
            *Both.scratch(s),
            *gather_sems(s.early),
        ],
    )(prod, w, h, wg, wd)


def back_kernel(s, dgu, w0, w1, w2, h, by, kept_g, kept_d, out, out_g, out_d, wv, local, kept, *refs):
    me = here()
    t = pl.program_id(0)
    both, terms = Both(s, me, out, *refs[:3]), Terms(s, me, s.kept, out_g, out_d, refs[3:])
    units = [w.at[u] for w in (w0, w1, w2) for u in range(w.shape[0])]
    loads = [pltpu.make_async_copy(one, wv.at[:, pl.ds(n * PAIR, PAIR)], local.at[n]) for n, one in enumerate(units)]

    each = len(units) // 3

    def third_of_first(n):
        for load in loads[n * each : (n + 1) * each]:
            load.wait()
        part = pl.ds(n * each * PAIR, each * PAIR)
        product = dot(dgu[:, part], wv[:, part], NT)
        both.total[...] = both.total[...] + product if n else product

    @pl.when(t == 0)
    def _():
        held = [pltpu.make_async_copy(src, term.at[v], sem) for v in range(s.kept) for term, src, sem in terms.kept(v, kept_g, kept_d, kept)]
        for load in loads[:each] + held + loads[each:]:
            load.start()
        greet(in_plane(me) + beside(me) + [twin(me)], lambda: third_of_first(0))
        for load in held:
            load.wait()

    terms.settle(t)

    @pl.when(t == 0)
    def _():
        third_of_first(1)
        third_of_first(2)

    def make(total):
        da = total.astype(bf16).astype(f32)
        wide = h[...].astype(f32)
        scale = lax.rsqrt(jnp.mean(wide * wide, -1, keepdims=True) + EPS)
        along = jnp.mean(da * wide, -1, keepdims=True)
        dh = (scale * da - wide * (scale * scale * scale * along)).astype(bf16)
        return (by[...].astype(f32) + dh.astype(f32)).astype(bf16)

    both.step(t, lambda: dot(dgu[...], wv[...], NT), make)


def back(s, dgu, w0, w1, w2, h, by, *kept):
    return call(
        functools.partial(back_kernel, s),
        "back",
        2,
        grid=(TILES + 1,),
        in_specs=[tile_spec(s, 2 * s.wide, 0), ANY, ANY, ANY, tile_spec(s, s.d, 1), tile_spec(s, s.d, 1), ANY, ANY],
        out_specs=[ANY] + [whole(one.shape) for one in sums(s, s.kept)],
        out_shape=[array(2, s.tokens, s.d), *sums(s, s.kept)],
        scratch_shapes=[
            pltpu.VMEM((s.d, 2 * s.wide), bf16),
            pltpu.SemaphoreType.DMA((2 * s.units,)),
            pltpu.SemaphoreType.DMA((s.kept, 4)),
            *Both.scratch(s),
            *terms_scratch(s, s.kept),
        ],
    )(dgu, w0, w1, w2, h, by, *kept)


def terms_scratch(s, units):
    return Scatter.scratch(s.pair, UNIT, units) * 2 + Scatter.scratch(s.sub, s.half, units) * 2


class Terms:
    def __init__(self, s, me, units, gates, downs, refs):
        self.s, self.units, self.gates, self.downs = s, units, gates, downs
        each = len(refs) // 4
        self.streams = [Scatter(me, refs[n * each : n * each + each - 2], *refs[n * each + each - 2 : n * each + each], *AXES[1 - n % 2]) for n in range(4)]

    def make(self, u, acts, dgu, prod, by, between=()):
        s, slot = self.s, lax.rem(u, 3)
        down = dot(prod[...], by[...], TN).astype(bf16)
        for n in range(2):
            self.streams[2 + n].term[slot] = down[:, n * s.half : (n + 1) * s.half].reshape(*PLANE, s.sub, s.half)
        for one in between:
            one.start()
        for k in range(2):
            both = dot(acts[:, k * s.half : (k + 1) * s.half], dgu[...], TN).astype(bf16)
            for n in range(2):
                self.streams[n].term[slot, HALVES[k]] = both[:, n * UNIT : (n + 1) * UNIT].reshape(2, 4, s.pair, UNIT)

    def put(self, n, u, value):
        s = self.s
        if n < 2:
            self.gates[u, :, :, pl.ds(n * UNIT, UNIT)] = value.reshape(2, s.rows, UNIT).astype(bf16)
        else:
            self.downs[u, :, pl.ds((n - 2) * (s.half), s.half)] = value.astype(bf16)

    def settle(self, j):
        for k in reversed(range(STAGES)):
            u = j - k

            @pl.when((u >= 0) & (u < self.units))
            def _(k=k, u=u):
                for m in ((0, 1), (2, 3)) if k == 0 else ():
                    for stream in self.streams:
                        stream.start(u, m)
                for n, stream in enumerate(self.streams if k else ()):
                    stream.stage(k, u, functools.partial(self.put, n))

    def kept(self, v, gates, downs, sems):
        return [(stream.term, (gates, downs)[n // 2].at[v, n % 2], sems.at[v, n]) for n, stream in enumerate(self.streams)]


def sums(s, units):
    return [array(units, 2, s.rows, PAIR), array(units, s.sub, s.d)]


def arrivals(s, sources, targets, sems):
    return [[pltpu.make_async_copy(src.at[part], dst.at[part], sems.at[n, m]) for m, (src, dst) in enumerate(zip(sources, targets, strict=True))] for n, part in enumerate(parts(s))]


def wait_first(j, arrive):
    @pl.when(j == 0)
    def _():
        for one in sum(arrive, []):
            one.wait()


def back_gates(both, by):
    gate, up, by = both[:, :UNIT], both[:, UNIT:], by.astype(f32)
    sig, act = silu_parts(gate)
    return (by * up * (sig + act * (1.0 - sig))).astype(bf16), (by * act).astype(bf16), (act * up).astype(bf16)


def second_kernel(s, acts_in, dys_in, wg, wd, g_early, d_early, dgux, g_late, theirs, kept_g, kept_d, out_g, out_d, acts, dys, gv, dv, dgu, prod, tiles_in, local, saved, given, sent, kept, *refs):
    me = here()
    j = pl.program_id(0)
    streams = streams_of(me, s, gv.at[pl.ds(2, s.late)], dv.at[pl.ds(2, s.late)], refs[:8])
    terms = Terms(s, me, s.summed, out_g, out_d, refs[8:])
    keeps = [[pltpu.make_async_copy(term.at[(s.summed + v) % 3], to, sem) for term, to, sem in terms.kept(v, kept_g, kept_d, kept)] for v in range(s.kept)]

    def at(k, u):
        at_stage(streams, k, u, s.late)

    def load(u):
        return [pltpu.make_async_copy(src.at[u], dst.at[flip(u)], local.at[n, flip(u)]) for n, (src, dst) in enumerate(((g_early, gv), (d_early, dv)))]

    arrive = arrivals(s, (acts_in, dys_in), (acts, dys), tiles_in)

    def place(u):
        return jnp.where(u < s.early, flip(u), u - s.early + 2)

    def save(u):
        return pltpu.make_async_copy(gv.at[place(u)], g_late.at[u - s.early], saved)

    def give(u):
        return remote(gv.at[place(u)], theirs.at[u], given.at[0, u], given.at[1, u], twin(me))

    def dgu_out(u):
        return split(s, me, dgu, dgux, u, PAIR, sent)

    @pl.when(j == 0)
    def _():
        y, z = me["y"], me["z"]
        rest = pl.ds(s.early, s.late)
        own = [pltpu.make_async_copy(src.at[1, rest], dst.at[pl.ds(2, s.late), y, z], local.at[2, n]) for n, (src, dst) in enumerate(((wg, gv), (wd, dv)))]
        for one in own + load(0) + load(1) + sum(arrive, []):
            one.start()
        greet(in_plane(me) + beside(me) + [twin(me)])
        for one in own:
            one.wait()
        early(streams, s.late, WARM[:1])

    for k in reversed(range(5)):
        at(k, j - k + 1)

    @pl.when((j >= 1) & (j <= s.units))
    def _():
        for one in (*dgu_out(j - 1), give(j - 1)):
            one.wait()

    @pl.when((j > s.early) & (j <= s.units))
    def _():
        save(j - 1).wait()

    @pl.when(j < s.units)
    def _():
        @pl.when(j < s.early)
        def _():
            for one in load(j):
                one.wait()

        @pl.when((j >= 1) & (j + 1 < s.early))
        def _():
            for one in load(j + 1):
                one.start()

        @pl.when(j >= s.early)
        def _():
            save(j).start()

        give(j).start()
        wait_first(j, arrive)
        now = place(j)
        weights, ahead = gv[now].reshape(s.d, PAIR), dv[now].reshape(UNIT, s.d)
        for part in parts(s):
            both = dot(acts[part], weights, NN)
            by = dot(dys[part], ahead, NT).astype(bf16)
            dgu[part, :UNIT], dgu[part, UNIT:], prod[part] = back_gates(both, by)
        terms.make(j, acts, dgu, prod, dys, dgu_out(j))

    for v, copies in enumerate(keeps):

        @pl.when(j == s.summed + v)
        def _(copies=copies):
            for one in copies:
                one.start()

    terms.settle(j)

    @pl.when(j == s.units)
    def _():
        for one in sum(keeps, []):
            one.wait()


def kept_shapes(s):
    return [array(s.kept, 2, *PLANE, s.pair, UNIT), array(s.kept, 2, *PLANE, s.sub, s.half)]


def second(s, acts, dys, wg, wd, g_early, d_early):
    unit, row = (*PLANE, s.pair, PAIR), (*PLANE, s.sub, s.d)
    return call(
        functools.partial(second_kernel, s),
        "second",
        3,
        grid=(s.summed + STAGES - 1,),
        in_specs=[ANY] * 6,
        out_specs=[ANY] * 5 + [whole(one.shape) for one in sums(s, s.summed)],
        out_shape=[array(s.tokens, 2 * s.wide), array(s.late, *unit), array(s.units, *unit), *kept_shapes(s), *sums(s, s.summed)],
        scratch_shapes=[
            *[pltpu.VMEM((s.both, s.d), bf16)] * 2,
            pltpu.VMEM((2 + s.late, *unit), bf16),
            pltpu.VMEM((2 + s.late, *row), bf16),
            pltpu.VMEM((s.both, PAIR), bf16),
            pltpu.VMEM((s.both, UNIT), bf16),
            pltpu.SemaphoreType.DMA((4, 2)),
            pltpu.SemaphoreType.DMA((3, 2)),
            pltpu.SemaphoreType.DMA,
            pltpu.SemaphoreType.DMA((2, s.units)),
            pltpu.SemaphoreType.DMA((3, s.units)),
            pltpu.SemaphoreType.DMA((s.kept, 4)),
            *gather_sems(s.late),
            *terms_scratch(s, s.summed),
        ],
    )(acts, dys, wg, wd, g_early, d_early)


def third_kernel(s, acts_in, dh_in, wd, gu, out_g, out_d, acts, dh, dgu, prod, tiles_in, *refs):
    me = here()
    j = pl.program_id(0)
    terms = Terms(s, me, s.units, out_g, out_d, refs)
    arrive = arrivals(s, (dh_in, acts_in), (dh, acts), tiles_in)

    @pl.when(j == 0)
    def _():
        for one in sum(arrive, []):
            one.start()
        greet(in_plane(me) + beside(me))

    @pl.when(j < s.units)
    def _():
        wait_first(j, arrive)
        ahead = wd[...]
        for part in parts(s):
            by = dot(dh[part], ahead, NT).astype(bf16)
            dgu[part, :UNIT], dgu[part, UNIT:], prod[part] = back_gates(gu[part], by)
        terms.make(j, acts, dgu, prod, dh)

    terms.settle(j)


def third(s, number, acts, dh, wd, gu):
    at = lambda j: jnp.minimum(j, s.units - 1)
    return call(
        functools.partial(third_kernel, s),
        "third",
        number,
        grid=(s.units + STAGES - 1,),
        in_specs=[ANY] * 2 + [pl.BlockSpec((UNIT, s.d), lambda j: (at(j), 0)), pl.BlockSpec((s.both, PAIR), lambda j: (0, at(j)))],
        out_specs=[whole(one.shape) for one in sums(s, s.units)],
        out_shape=sums(s, s.units),
        scratch_shapes=[
            *[pltpu.VMEM((s.both, s.d), bf16)] * 2,
            pltpu.VMEM((s.both, PAIR), bf16),
            pltpu.VMEM((s.both, UNIT), bf16),
            pltpu.SemaphoreType.DMA((4, 2)),
            *terms_scratch(s, s.units),
        ],
    )(acts, dh, wd, gu)


def adamw(w, m, v, g):
    m = 0.9 * m + 0.1 * g
    v = 0.95 * v + 0.05 * g * g
    step = m * lax.rsqrt(v + 1e-8) + 0.1 * w
    return (w - 0.02 * step).astype(bf16), m, v


def others(me):
    steps = [(y, z, c) for y in range(4) for z in range(4) for c in range(2)]
    return [{"y": ring(me["y"], y), "z": ring(me["z"], z), "c": flip(me["c"] + c)} for y, z, c in steps[1:]]


def total_kernel(s, g0, d0, g1, d1, g2, d2, out, squares, sums, got0, got1, got2, sent, here_got):
    me = here()
    c = me["c"]

    def add_up():
        total = sum(jnp.sum(g[...].astype(f32) ** 2) for g in (g0, d0, g1, d1, g2, d2))
        sums[0] = jnp.full(squares.shape, total)

    greet(others(me), add_up)
    exchanged = (g0, got0), (g1, got1), (g2, got2)
    pairs = [remote(g.at[:, 1 - c], got, sent.at[n], here_got.at[n], twin(me)) for n, (g, got) in enumerate(exchanged)]
    for one in pairs:
        one.start()
    copies = [remote(sums.at[0], sums.at[n], sent.at[n + 2], here_got.at[n + 2], to) for n, to in enumerate(others(me), 1)]
    for one in copies:
        one.start()
    for one in pairs:
        one.wait()
    moves = [(start, n, core * s.ff + to) for core in range(2) for to, n, start in places(s, core)]
    for layer, refs in enumerate((exchanged[:1], exchanged[1:])):
        for mat in range(2):
            lanes = pl.ds(mat * UNIT, UNIT)
            mine = jnp.concatenate([g[u, c, :, lanes] for g, _ in refs for u in range(g.shape[0])], 1).astype(f32)
            other = jnp.concatenate([got[u, :, lanes] for _, got in refs for u in range(got.shape[0])], 1).astype(f32)
            both = jnp.concatenate([jnp.where(c == 0, mine, other), jnp.where(c == 0, other, mine)], 1)
            out[layer, mat] = jnp.concatenate(tiles(both, 32 * s.block, moves), 1).astype(bf16)
    for one in copies:
        one.wait()
    squares[...] = jnp.sum(sums[...], 0)


def total(s, number, *sums):
    tile = (8, HALF)
    sems = pltpu.SemaphoreType.DMA((34,))
    return call(
        functools.partial(total_kernel, s),
        "total",
        number,
        in_specs=[VMEM] * 6,
        out_specs=[VMEM] * 2,
        out_shape=[array(s.layers, 2, s.rows, 32 * s.block), array(*tile, dtype=f32)],
        scratch_shapes=[pltpu.VMEM((32, *tile), f32), *[pltpu.VMEM((g.shape[0], *g.shape[2:]), bf16) for g in sums[::2]], sems, sems],
    )(*sums)


def finish_kernel(s, g, d0, d1, d2, squares, *refs):
    old, new, bufs, (ins, outs) = refs[:9], refs[9:18], refs[18:27], refs[27:]
    loads = [pltpu.make_async_copy(src, dst, ins.at[n]) for n, (src, dst) in enumerate(zip(old, bufs, strict=True))]
    stores = [pltpu.make_async_copy(src, dst, outs.at[n]) for n, (src, dst) in enumerate(zip(bufs, new, strict=True))]
    for n in range(3):
        for load in loads[n::3]:
            load.start()
    count = s.layers * s.d * 32 * s.block * 3
    factor = jnp.minimum(1.0, 0.5 * lax.rsqrt(squares[:1, :1] / count + 1e-30))
    for n in range(3):
        for load in loads[n::3]:
            load.wait()
        for layer in range(s.layers):
            if n < 2:
                at, grad = layer, g[layer, n].astype(f32)
            else:
                rows = jnp.concatenate([one[...] for one in ((d1, d2) if layer else (d0,))], 0).reshape(s.padded, s.d)
                at, grad = (slice(None), layer), rows[: s.block].astype(f32)
            w, m, v = bufs[n::3]
            made = adamw(w[at].astype(f32), m[at], v[at], grad * factor)
            for ref, value in zip((w, m, v), made, strict=True):
                ref[at] = value
        for store in stores[n::3]:
            store.start()
    for store in stores:
        store.wait()


def finish(s, g, downs, squares, old):
    out = [array(*one.shape, dtype=one.dtype) for one in old]
    sems = pltpu.SemaphoreType.DMA((9,))
    kernel = functools.partial(finish_kernel, s)
    scratch = [pltpu.VMEM(one.shape, one.dtype) for one in old] + [sems, sems]
    return call(kernel, "finish", None, in_specs=[VMEM] * 5 + [ANY] * 9, out_specs=[ANY] * 9, out_shape=out, scratch_shapes=scratch)(g, *downs, squares, *old)


def turned(arrays):
    return [one.swapaxes(0, 1) if n % 3 == 2 else one for n, one in enumerate(arrays)]


def solution(mesh):
    cut_mesh = Mesh(mesh.devices.reshape(mesh.shape["rep"], mesh.shape["r"], 4, 4, 2), ("rep", "x", "y", "z", "c"))

    def step(x, dy, *arrays):
        s = sizes(x.shape, arrays[0].shape, arrays[2].shape)
        arrays = turned(arrays)
        flat = (s.both, s.d)
        gates, downs = prepare(s, arrays[:3])
        gates = gates.reshape(s.layers, s.units, s.pair, PAIR)
        downs = downs.reshape(s.layers, s.units, s.sub, s.d)
        acts0, dys, gu0, prod0, wd0 = first(s, x[0], dy[0], gates, downs)
        h1, acts1, g_early, d_early = down(s, prod0, wd0.reshape(s.wide, s.d), x[0], gates, downs)
        dys, acts0, acts1 = (one.reshape(flat) for one in (dys, acts0, acts1))
        dgu1, g_late, theirs, kept_g, kept_d, *sums1 = second(s, acts1, dys, gates, downs, g_early, d_early)
        w = (one.reshape(-1, s.d, PAIR) for one in (g_early, g_late, theirs))
        dh, *sums2 = back(s, dgu1, *w, h1, dy[0], kept_g, kept_d)
        dh = dh.reshape(flat)
        sums0 = third(s, 6, acts0, dh, wd0.reshape(-1, s.d), gu0)
        every = (*sums0, *sums1, *sums2)
        g, squares = total(s, 7, *every)
        return tuple(turned(finish(s, g, every[1::2], squares, arrays)))

    place = ("y", "z", "c")
    states, cut = P(("rep", "x", *place), None, None), P(None, place, None)
    return jax.shard_map(
        step,
        mesh=cut_mesh,
        in_specs=(states, states) + (cut,) * 9,
        out_specs=(P("rep", place, None),) * 9,
        check_vma=False,
    )
```
